8 devices in a mesh: data: 1 (over z), cp: 8 (over y, x, core).
Axes of the slice: x: 2, y: 2, z: 1, core: 2. Of those that a mesh axis runs over, the one named last changes fastest.
Arguments:
- q: bfloat16 [1, 4096, 96, 128], P('data', 'cp')
- k: bfloat16 [1, 4096, 96, 128], P('data', 'cp')
- v: bfloat16 [1, 4096, 96, 128], P('data', 'cp')
- o: bfloat16 [1, 4096, 96, 128], P('data', 'cp')
- lse: float32 [1, 96, 4096], P('data', None, 'cp')
- do: bfloat16 [1, 4096, 96, 128], P('data', 'cp')
Outputs:
- output 1: bfloat16 [1, 4096, 96, 128], P('data', 'cp')
- output 2: bfloat16 [1, 4096, 96, 128], P('data', 'cp')
- output 3: bfloat16 [1, 4096, 96, 128], P('data', 'cp')
All inputs are finite; a program needn't handle non-finite values.
Results may differ from the reference program's by a relative error of at most 0.001.
Values are sent between devices in bfloat16 or wider.
A program may use at most 1 GiB of HBM per device.

```python
import jax
import jax.numpy as jnp
from jax import lax
import numpy as np

CP = 8
BATCH = 1
TOKENS_DEV = 512
HEADS = 96
HEAD = 128


def _positions():
    c = TOKENS_DEV // 2
    dev = np.arange(CP)[:, None]
    u = np.arange(c)[None, :]
    return np.concatenate([dev * c + u, (2 * CP - 1 - dev) * c + u], axis=1).reshape(2 * CP, c)


def _segments(x):
    c = TOKENS_DEV // 2
    return jnp.moveaxis(x.astype(jnp.float32).reshape(BATCH, 2 * CP, c, HEADS, HEAD), 1, 0)


def _forward(q, k, v):
    c = TOKENS_DEV // 2
    scale = HEAD ** -0.5
    pos = jnp.asarray(_positions(), dtype=jnp.int32)
    qs, ks, vs = _segments(q), _segments(k), _segments(v)

    def one(xs):
        qb, pq = xs

        def scores(kb, pk):
            s = jnp.einsum('bqhd,bkhd->bhqk', qb, kb) * scale
            return jnp.where(pq[:, None] >= pk[None, :], s, -jnp.inf)

        def stat(carry, ys):
            m, l = carry
            s = scores(*ys)
            m2 = jnp.maximum(m, jnp.max(s, axis=-1))
            return (m2, l * jnp.exp(m - m2) + jnp.sum(jnp.exp(s - m2[..., None]), axis=-1)), None

        m0 = jnp.full((BATCH, HEADS, c), -jnp.inf, jnp.float32)
        (m, l), _ = lax.scan(stat, (m0, jnp.zeros_like(m0)), (ks, pos))
        lse = m + jnp.log(l)

        def acc(o, ys):
            kb, vb, pk = ys
            p = jnp.exp(scores(kb, pk) - lse[..., None])
            return o + jnp.einsum('bhqk,bkhd->bqhd', p, vb), None

        o, _ = lax.scan(acc, jnp.zeros((BATCH, c, HEADS, HEAD), jnp.float32), (ks, vs, pos))
        return o, lse

    o, lse = lax.map(one, (qs, pos))
    o = jnp.moveaxis(o, 0, 1).reshape(BATCH, CP * TOKENS_DEV, HEADS, HEAD).astype(jnp.bfloat16)
    lse = jnp.moveaxis(lse, 0, 2).reshape(BATCH, HEADS, CP * TOKENS_DEV)
    return o, lse


def setup_inputs(seed: int = 0, part: int = 0) -> dict:
    key = jax.random.fold_in(jax.random.PRNGKey(seed), part)
    kq, kk, kv, kd = jax.random.split(key, 4)
    shape = (BATCH, CP * TOKENS_DEV, HEADS, HEAD)
    q = jax.random.normal(kq, shape, jnp.float32).astype(jnp.bfloat16)
    k = jax.random.normal(kk, shape, jnp.float32).astype(jnp.bfloat16)
    v = jax.random.normal(kv, shape, jnp.float32).astype(jnp.bfloat16)
    do = jax.random.normal(kd, shape, jnp.float32).astype(jnp.bfloat16)
    o, lse = _forward(q, k, v)
    return {'q': q, 'k': k, 'v': v, 'o': o, 'lse': lse, 'do': do}


def reference(q, k, v, o, lse, do):
    nseg = 2 * CP
    c = TOKENS_DEV // 2
    scale = HEAD ** -0.5
    pos = jnp.asarray(_positions(), dtype=jnp.int32)
    qs, ks, vs, dos = _segments(q), _segments(k), _segments(v), _segments(do)
    delta = jnp.sum(do.astype(jnp.float32) * o.astype(jnp.float32), axis=-1)
    deltas = jnp.moveaxis(jnp.swapaxes(delta, 1, 2).reshape(BATCH, HEADS, nseg, c), 2, 0)
    lses = jnp.moveaxis(lse.reshape(BATCH, HEADS, nseg, c), 2, 0)

    def per_query(carry, xs):
        dk, dv = carry
        qb, dob, lb, db, pq = xs

        def per_key(ys):
            kb, vb, pk = ys
            s = jnp.einsum('bqhd,bkhd->bhqk', qb, kb) * scale
            p = jnp.where(pq[:, None] >= pk[None, :], jnp.exp(s - lb[..., None]), 0.0)
            dvb = jnp.einsum('bhqk,bqhd->bkhd', p.astype(jnp.bfloat16).astype(jnp.float32), dob)
            dp = jnp.einsum('bqhd,bkhd->bhqk', dob, vb)
            ds = (p * (dp - db[..., None])).astype(jnp.bfloat16).astype(jnp.float32)
            return jnp.einsum('bhqk,bkhd->bqhd', ds, kb), jnp.einsum('bhqk,bqhd->bkhd', ds, qb), dvb

        dqs, dks, dvs = lax.map(per_key, (ks, vs, pos))
        return (dk + dks, dv + dvs), jnp.sum(dqs, axis=0)

    zero = jnp.zeros_like(ks)
    (dk, dv), dq = lax.scan(per_query, (zero, zero), (qs, dos, lses, deltas, pos))

    def unseg(x):
        return jnp.moveaxis(x, 0, 1).reshape(BATCH, CP * TOKENS_DEV, HEADS, HEAD).astype(jnp.bfloat16)

    return unseg(dq * scale), unseg(dk * scale), unseg(dv)
```

```python
import functools

import jax
import jax.numpy as jnp
from jax import lax
from jax.experimental import pallas as pl
from jax.experimental.pallas import tpu as pltpu
from jax.sharding import PartitionSpec as P

F32 = jnp.float32
BF16 = jnp.bfloat16
MESH = pl.DeviceIdType.MESH

NT = (((1,), (1,)), ((), ()))
NN = (((1,), (0,)), ((), ()))


def _dot(a, b, dims):
    return lax.dot_general(a, b, dims, preferred_element_type=F32)


def _kernel(n, toks, heads, q_ref, k_ref, v_ref, o_ref, do_ref, lse_ref, dq_ref, dk_ref, dv_ref,
            raw, raw_lse, snd, snd_st, rcv, rcv_st, osnd, orcv, ostage, tmp, kt, dqt, dka, dva,
            isend, irecv, ssend, srecv, osend, orecv, ldsem, lsesem, stsem):
    half = toks // 2
    d = q_ref.shape[-1]
    scale = d ** -0.5
    chunks = heads // n
    me = lax.axis_index('cp')
    row = lax.axis_index('data')

    def peer(r):
        p = me
        if r & 1:
            p = p + 1 - 2 * lax.rem(me, 2)
        if r & 2:
            p = p + 2 - 4 * lax.rem(me // 2, 2)
        if r & 4:
            p = p + 4 - 8 * lax.rem(me // 4, 2)
        return p

    barrier = pltpu.get_barrier_semaphore()
    for r in range(1, n):
        pl.semaphore_signal(barrier, inc=1, device_id=(row, peer(r)), device_id_type=MESH)
    pl.semaphore_wait(barrier, n - 1)

    srcs = (q_ref, k_ref, v_ref, do_ref, o_ref)
    dsts = (dq_ref, dk_ref, dv_ref)

    def loads(c):
        h = pl.ds(pl.multiple_of(c * n, n), n)
        out = [pltpu.make_async_copy(x.at[:, h, :], raw.at[a], ldsem.at[a]) for a, x in enumerate(srcs)]
        out.append(pltpu.make_async_copy(lse_ref.at[h, :], raw_lse, lsesem))
        return out

    def stores(c):
        h = pl.ds(pl.multiple_of(c * n, n), n)
        return [pltpu.make_async_copy(ostage.at[a], x.at[:, h, :], stsem.at[a]) for a, x in enumerate(dsts)]

    def remote(src, dst, ssem, rsem, p):
        return pltpu.make_async_remote_copy(src_ref=src, dst_ref=dst, send_sem=ssem, recv_sem=rsem,
                                            device_id=(row, p), device_id_type=MESH)

    def in_copies(s, r, at):
        p = peer(r)
        a, b, par = lax.rem(s, 2), lax.rem(s, 3), lax.rem(s, 2)
        return (remote(snd.at[a, p], rcv.at[b, at], isend.at[r], irecv.at[par, r], p),
                remote(snd_st.at[a, p], rcv_st.at[b, at], ssend.at[r], srecv.at[par, r], p))

    def out_copies(s, r, at):
        p = peer(r)
        c = s - 2
        a, b, par = lax.rem(c, 2), lax.rem(c, 3), lax.rem(c, 2)
        return (remote(osnd.at[a, p], orcv.at[b, at], osend.at[r], orecv.at[par, r], p),)

    def prepare(c):
        a_slot = lax.rem(c, 2)
        part = toks // 4

        def tensor(a, _):
            def piece(i, _):
                rows = pl.ds(pl.multiple_of(i * part, part), part)
                x = raw[a, rows].astype(F32).reshape(part * n, d)
                tmp[pl.ds(0, part * n), :] = x
                for h in range(n):
                    snd[a_slot, h, pl.ds(pl.multiple_of(a * toks + i * part, part), part), :] = (
                        tmp[pl.ds(h, part, stride=n), :].astype(BF16))
                return 0
            return lax.fori_loop(0, 4, piece, 0)
        lax.fori_loop(0, 4, tensor, 0)

        def stat(i, _):
            rows = pl.ds(pl.multiple_of(i * part, part), part)
            x = raw[3, rows].astype(F32) * raw[4, rows].astype(F32)
            tmp[pl.ds(0, part * n), :] = x.reshape(part * n, d)
            for h in range(n):
                y = tmp[pl.ds(h, part, stride=n), :]
                snd_st[a_slot, h, 1:2, pl.ds(pl.multiple_of(i * part, part), part)] = (
                    jnp.sum(y.T, axis=0, keepdims=True))
            return 0
        lax.fori_loop(0, 4, stat, 0)
        for h in range(n):
            snd_st[a_slot, h, 0:1, :] = raw_lse[h:h + 1, :]

    def finalize(c):
        b_slot = lax.rem(c, 3)
        part = toks // 4

        def tensor(a, _):
            def piece(i, _):
                rows = pl.ds(pl.multiple_of(i * part, part), part)
                for h in range(n):
                    tmp[pl.ds(h, part, stride=n), :] = (
                        orcv[b_slot, h, pl.ds(pl.multiple_of(a * toks + i * part, part), part), :].astype(F32))
                ostage[a, rows] = tmp[pl.ds(0, part * n), :].reshape(part, n, d).astype(BF16)
                return 0
            return lax.fori_loop(0, 4, piece, 0)
        lax.fori_loop(0, 3, tensor, 0)

    def tile(b, i, q0, qn, j, k0, kn, mask):
        q = rcv[b, i, q0:q0 + qn, :]
        k = rcv[b, j, toks + k0:toks + k0 + kn, :]
        v = rcv[b, j, 2 * toks + k0:2 * toks + k0 + kn, :]
        do = rcv[b, i, 3 * toks + q0:3 * toks + q0 + qn, :]
        lse = rcv_st[b, i, 0:1, q0:q0 + qn]
        delta = rcv_st[b, i, 1:2, q0:q0 + qn]
        p = jnp.exp(_dot(k, q, NT) * scale - lse)
        if mask is not None:
            p = jnp.where(mask, p, 0.0)
        dp = _dot(v, do, NT)
        ds = (p * (dp - delta)).astype(BF16)
        dva[j, k0:k0 + kn, :] += _dot(p.astype(BF16), do, NN)
        dka[j, k0:k0 + kn, :] += _dot(ds, q, NN)
        dqt[i, :, q0:q0 + qn] += _dot(kt[j, :, k0:k0 + kn], ds, NN)

    def compute(c):
        b = lax.rem(c, 3)
        oslot = lax.rem(c, 2)

        def clear(j, _):
            kt[j] = rcv[b, j, toks:2 * toks, :].T
            dqt[j] = jnp.zeros((d, toks), F32)
            dka[j] = jnp.zeros((toks, d), F32)
            dva[j] = jnp.zeros((toks, d), F32)
            return 0
        lax.fori_loop(0, n, clear, 0)

        tri = (lax.broadcasted_iota(jnp.int32, (half, half), 0)
               <= lax.broadcasted_iota(jnp.int32, (half, half), 1))

        def keys(j, _):
            tile(b, j, 0, half, j, 0, half, tri)
            tile(b, j, half, half, j, 0, half, None)
            tile(b, j, half, half, j, half, half, tri)

            def lower(i, _):
                tile(b, i, half, half, j, 0, toks, None)
                return 0
            lax.fori_loop(0, j, lower, 0)

            def higher(i, _):
                tile(b, i, 0, toks, j, 0, half, None)
                return 0
            lax.fori_loop(j + 1, n, higher, 0)
            osnd[oslot, j, toks:2 * toks, :] = (dka[j] * scale).astype(BF16)
            osnd[oslot, j, 2 * toks:3 * toks, :] = dva[j].astype(BF16)
            return 0
        lax.fori_loop(0, n, keys, 0)

        def finish(i, _):
            osnd[oslot, i, 0:toks, :] = (dqt[i].T * scale).astype(BF16)
            return 0
        lax.fori_loop(0, n, finish, 0)

    for x in loads(0):
        x.start()
    for x in loads(0):
        x.wait()
    prepare(0)
    for x in loads(1):
        x.start()

    def step(s, _):
        sends_in = s < chunks
        sends_out = (s >= 2) & (s < chunks + 2)

        @pl.when(sends_in)
        def _():
            for r in (2, 4, 3, 5):
                for x in in_copies(s, r, me):
                    x.start()

        @pl.when(sends_out)
        def _():
            for r in (2, 4, 3, 5):
                for x in out_copies(s, r, me):
                    x.start()

        @pl.when(sends_in)
        def _():
            for r in (1, 6, 7):
                for x in in_copies(s, r, me):
                    x.start()
            a, b = lax.rem(s, 2), lax.rem(s, 3)
            rcv[b, me] = snd[a, me]
            rcv_st[b, me] = snd_st[a, me]

        @pl.when(sends_out)
        def _():
            for r in (1, 6, 7):
                for x in out_copies(s, r, me):
                    x.start()
            a, b = lax.rem(s - 2, 2), lax.rem(s - 2, 3)
            orcv[b, me] = osnd[a, me]

        @pl.when(s >= 4)
        def _():
            for x in stores(s - 4):
                x.start()

        @pl.when((s >= 1) & (s < chunks + 1))
        def _():
            compute(s - 1)

        @pl.when(s + 1 < chunks)
        def _():
            for x in loads(s + 1):
                x.wait()
            prepare(s + 1)

        @pl.when(s + 2 < chunks)
        def _():
            for x in loads(s + 2):
                x.start()

        @pl.when(s >= 4)
        def _():
            for x in stores(s - 4):
                x.wait()

        @pl.when(s >= 3)
        def _():
            finalize(s - 3)

        @pl.when(sends_in)
        def _():
            for r in range(1, n):
                for x in in_copies(s, r, me):
                    x.wait_send()
                for x in in_copies(s, r, peer(r)):
                    x.wait_recv()

        @pl.when(sends_out)
        def _():
            for r in range(1, n):
                for x in out_copies(s, r, me):
                    x.wait_send()
                for x in out_copies(s, r, peer(r)):
                    x.wait_recv()
        return 0

    lax.fori_loop(0, chunks + 3, step, 0)
    for x in stores(chunks - 1):
        x.start()
    for x in stores(chunks - 1):
        x.wait()


def solution(mesh):
    n = mesh.shape['cp']
    spec = P('data', 'cp', None, None)
    lspec = P('data', None, 'cp')

    def local(q, k, v, o, lse, do):
        _, toks, heads, d = q.shape
        out = jax.ShapeDtypeStruct((toks, heads, d), BF16)
        any_ = pl.BlockSpec(memory_space=pl.ANY)
        dma = pltpu.SemaphoreType.DMA
        dq, dk, dv = pl.pallas_call(
            functools.partial(_kernel, n, toks, heads),
            out_shape=(out, out, out),
            in_specs=[any_] * 6,
            out_specs=(any_,) * 3,
            scratch_shapes=[
                pltpu.VMEM((5, toks, n, d), BF16),
                pltpu.VMEM((n, toks), F32),
                pltpu.VMEM((2, n, 4 * toks, d), BF16),
                pltpu.VMEM((2, n, 2, toks), F32),
                pltpu.VMEM((3, n, 4 * toks, d), BF16),
                pltpu.VMEM((3, n, 2, toks), F32),
                pltpu.VMEM((2, n, 3 * toks, d), BF16),
                pltpu.VMEM((3, n, 3 * toks, d), BF16),
                pltpu.VMEM((3, toks, n, d), BF16),
                pltpu.VMEM((toks // 4 * n, d), F32),
                pltpu.VMEM((n, d, toks), BF16),
                pltpu.VMEM((n, d, toks), F32),
                pltpu.VMEM((n, toks, d), F32),
                pltpu.VMEM((n, toks, d), F32),
                dma((n,)), dma((2, n)), dma((n,)), dma((2, n)), dma((n,)), dma((2, n)),
                dma((5,)), dma, dma((3,)),
            ],
            compiler_params=pltpu.CompilerParams(
                collective_id=0, has_side_effects=True, vmem_limit_bytes=67_043_328),
        )(q[0], k[0], v[0], o[0], do[0], lse[0])
        return dq[None], dk[None], dv[None]

    return jax.shard_map(local, mesh=mesh, in_specs=(spec, spec, spec, spec, lspec, spec),
                         out_specs=(spec, spec, spec), check_vma=False)
```

```python
import functools

import jax
import jax.numpy as jnp
from jax import lax
from jax.experimental import pallas as pl
from jax.experimental.pallas import tpu as pltpu
from jax.sharding import PartitionSpec as P

F32 = jnp.float32
BF16 = jnp.bfloat16
MESH = pl.DeviceIdType.MESH

NT = (((1,), (1,)), ((), ()))
NN = (((1,), (0,)), ((), ()))


def _dot(a, b, dims):
    return lax.dot_general(a, b, dims, preferred_element_type=F32)


def _kernel(n, toks, heads, q_ref, k_ref, v_ref, o_ref, do_ref, lse_ref, dq_ref, dk_ref, dv_ref,
            raw, raw_lse, snd, snd_st, rcv, rcv_st, osnd, orcv, ostage, tmp, kt, dqt, dka, dva,
            isend, irecv, ssend, srecv, osend, orecv, ldsem, lsesem, stsem):
    half = toks // 2
    d = q_ref.shape[-1]
    scale = d ** -0.5
    chunks = heads // n
    me = lax.axis_index('cp')
    row = lax.axis_index('data')

    def peer(r):
        p = me
        if r & 1:
            p = p + 1 - 2 * lax.rem(me, 2)
        if r & 2:
            p = p + 2 - 4 * lax.rem(me // 2, 2)
        if r & 4:
            p = p + 4 - 8 * lax.rem(me // 4, 2)
        return p

    srcs = (q_ref, k_ref, v_ref, do_ref, o_ref)
    dsts = (dq_ref, dk_ref, dv_ref)

    def loads(c):
        h = pl.ds(pl.multiple_of(c * n, n), n)
        out = [pltpu.make_async_copy(x.at[:, h, :], raw.at[a], ldsem.at[a]) for a, x in enumerate(srcs)]
        out.append(pltpu.make_async_copy(lse_ref.at[h, :], raw_lse, lsesem))
        return out

    def stores(c):
        h = pl.ds(pl.multiple_of(c * n, n), n)
        return [pltpu.make_async_copy(ostage.at[a], x.at[:, h, :], stsem.at[a]) for a, x in enumerate(dsts)]

    def remote(src, dst, ssem, rsem, p):
        return pltpu.make_async_remote_copy(src_ref=src, dst_ref=dst, send_sem=ssem, recv_sem=rsem,
                                            device_id=(row, p), device_id_type=MESH)

    def in_copies(s, r, at):
        p = peer(r)
        a, b, par = lax.rem(s, 2), lax.rem(s, 3), lax.rem(s, 2)
        return (remote(snd.at[a, p], rcv.at[b, at], isend.at[r], irecv.at[par, r], p),
                remote(snd_st.at[a, p], rcv_st.at[b, at], ssend.at[r], srecv.at[par, r], p))

    def out_copies(c, r, at):
        p = peer(r)
        a, b, par = lax.rem(c, 2), lax.rem(c, 3), lax.rem(c, 2)
        return (remote(osnd.at[a, p], orcv.at[b, at], osend.at[r], orecv.at[par, r], p),)

    def prepare(c):
        a_slot = lax.rem(c, 2)
        part = toks // 4

        def tensor(a, _):
            def piece(i, _):
                rows = pl.ds(pl.multiple_of(i * part, part), part)
                x = raw[a, rows].astype(F32).reshape(part * n, d)
                tmp[pl.ds(0, part * n), :] = x
                for h in range(n):
                    snd[a_slot, h, pl.ds(pl.multiple_of(a * toks + i * part, part), part), :] = (
                        tmp[pl.ds(h, part, stride=n), :].astype(BF16))
                return 0
            return lax.fori_loop(0, 4, piece, 0)
        lax.fori_loop(0, 4, tensor, 0)

        def stat(i, _):
            rows = pl.ds(pl.multiple_of(i * part, part), part)
            x = raw[3, rows].astype(F32) * raw[4, rows].astype(F32)
            tmp[pl.ds(0, part * n), :] = x.reshape(part * n, d)
            for h in range(n):
                y = tmp[pl.ds(h, part, stride=n), :]
                snd_st[a_slot, h, 1:2, pl.ds(pl.multiple_of(i * part, part), part)] = (
                    jnp.sum(y.T, axis=0, keepdims=True))
            return 0
        lax.fori_loop(0, 4, stat, 0)
        for h in range(n):
            snd_st[a_slot, h, 0:1, :] = raw_lse[h:h + 1, :]

    def finalize(c):
        b_slot = lax.rem(c, 3)
        part = toks // 4

        def tensor(a, _):
            def piece(i, _):
                rows = pl.ds(pl.multiple_of(i * part, part), part)
                for h in range(n):
                    tmp[pl.ds(h, part, stride=n), :] = (
                        orcv[b_slot, h, pl.ds(pl.multiple_of(a * toks + i * part, part), part), :].astype(F32))
                ostage[a, rows] = tmp[pl.ds(0, part * n), :].reshape(part, n, d).astype(BF16)
                return 0
            return lax.fori_loop(0, 4, piece, 0)
        lax.fori_loop(0, 3, tensor, 0)

    def tile(b, i, q0, qn, j, k0, kn, mask):
        q = rcv[b, i, q0:q0 + qn, :]
        k = rcv[b, j, toks + k0:toks + k0 + kn, :]
        v = rcv[b, j, 2 * toks + k0:2 * toks + k0 + kn, :]
        do = rcv[b, i, 3 * toks + q0:3 * toks + q0 + qn, :]
        lse = rcv_st[b, i, 0:1, q0:q0 + qn]
        delta = rcv_st[b, i, 1:2, q0:q0 + qn]
        p = jnp.exp(_dot(k, q, NT) * scale - lse)
        if mask is not None:
            p = jnp.where(mask, p, 0.0)
        dp = _dot(v, do, NT)
        ds = (p * (dp - delta)).astype(BF16)
        dva[j, k0:k0 + kn, :] += _dot(p.astype(BF16), do, NN)
        dka[j, k0:k0 + kn, :] += _dot(ds, q, NN)
        dqt[i, :, q0:q0 + qn] += _dot(kt[j, :, k0:k0 + kn], ds, NN)

    def begin(c):
        b = lax.rem(c, 3)

        def clear(j, _):
            kt[j] = rcv[b, j, toks:2 * toks, :].T
            dqt[j] = jnp.zeros((d, toks), F32)
            dka[j] = jnp.zeros((toks, d), F32)
            dva[j] = jnp.zeros((toks, d), F32)
            return 0
        lax.fori_loop(0, n, clear, 0)

    def compute(c, lo, hi):
        b = lax.rem(c, 3)
        tri = (lax.broadcasted_iota(jnp.int32, (half, half), 0)
               <= lax.broadcasted_iota(jnp.int32, (half, half), 1))

        def keys(j, _):
            tile(b, j, 0, half, j, 0, half, tri)
            tile(b, j, half, half, j, 0, half, None)
            tile(b, j, half, half, j, half, half, tri)

            def lower(i, _):
                tile(b, i, half, half, j, 0, toks, None)
                return 0
            lax.fori_loop(0, j, lower, 0)

            def higher(i, _):
                tile(b, i, 0, toks, j, 0, half, None)
                return 0
            lax.fori_loop(j + 1, n, higher, 0)
            return 0
        lax.fori_loop(lo, hi, keys, 0)

    def finish(c):
        oslot = lax.rem(c, 2)

        def block(i, _):
            osnd[oslot, i, 0:toks, :] = (dqt[i].T * scale).astype(BF16)
            osnd[oslot, i, toks:2 * toks, :] = (dka[i] * scale).astype(BF16)
            osnd[oslot, i, 2 * toks:3 * toks, :] = dva[i].astype(BF16)
            return 0
        lax.fori_loop(0, n, block, 0)

    for x in loads(0):
        x.start()
    barrier = pltpu.get_barrier_semaphore()
    for r in range(1, n):
        pl.semaphore_signal(barrier, inc=1, device_id=(row, peer(r)), device_id_type=MESH)
    for x in loads(0):
        x.wait()
    prepare(0)
    for x in loads(1):
        x.start()
    pl.semaphore_wait(barrier, n - 1)

    order = (2, 4, 3, 5, 1, 6, 7)

    def begin_in(s):
        for r in order:
            for x in in_copies(s, r, me):
                x.start()
        a, b = lax.rem(s, 2), lax.rem(s, 3)
        rcv[b, me] = snd[a, me]
        rcv_st[b, me] = snd_st[a, me]

    def end_in(s):
        for r in range(1, n):
            for x in in_copies(s, r, me):
                x.wait_send()
            for x in in_copies(s, r, peer(r)):
                x.wait_recv()

    def begin_out(c):
        for r in order:
            for x in out_copies(c, r, me):
                x.start()
        a, b = lax.rem(c, 2), lax.rem(c, 3)
        orcv[b, me] = osnd[a, me]

    def end_out(c):
        for r in range(1, n):
            for x in out_copies(c, r, me):
                x.wait_send()
            for x in out_copies(c, r, peer(r)):
                x.wait_recv()

    def step(s, _):
        computes = (s >= 1) & (s < chunks + 1)

        @pl.when(computes)
        def _():
            end_in(s - 1)

        @pl.when(s < chunks)
        def _():
            begin_in(s)

        @pl.when(s >= 4)
        def _():
            for x in stores(s - 4):
                x.start()

        @pl.when(computes)
        def _():
            begin(s - 1)
            compute(s - 1, 0, n // 2)

        @pl.when(s >= 3)
        def _():
            end_out(s - 3)

        @pl.when((s >= 2) & (s < chunks + 2))
        def _():
            begin_out(s - 2)

        @pl.when(computes)
        def _():
            compute(s - 1, n // 2, n)
            finish(s - 1)

        @pl.when(s + 1 < chunks)
        def _():
            for x in loads(s + 1):
                x.wait()
            prepare(s + 1)

        @pl.when(s + 2 < chunks)
        def _():
            for x in loads(s + 2):
                x.start()

        @pl.when(s >= 4)
        def _():
            for x in stores(s - 4):
                x.wait()

        @pl.when(s >= 3)
        def _():
            finalize(s - 3)
        return 0

    lax.fori_loop(0, chunks + 3, step, 0)
    for x in stores(chunks - 1):
        x.start()
    for x in stores(chunks - 1):
        x.wait()


def solution(mesh):
    n = mesh.shape['cp']
    spec = P('data', 'cp', None, None)
    lspec = P('data', None, 'cp')

    def local(q, k, v, o, lse, do):
        _, toks, heads, d = q.shape
        out = jax.ShapeDtypeStruct((toks, heads, d), BF16)
        any_ = pl.BlockSpec(memory_space=pl.ANY)
        dma = pltpu.SemaphoreType.DMA
        dq, dk, dv = pl.pallas_call(
            functools.partial(_kernel, n, toks, heads),
            out_shape=(out, out, out),
            in_specs=[any_] * 6,
            out_specs=(any_,) * 3,
            scratch_shapes=[
                pltpu.VMEM((5, toks, n, d), BF16),
                pltpu.VMEM((n, toks), F32),
                pltpu.VMEM((2, n, 4 * toks, d), BF16),
                pltpu.VMEM((2, n, 2, toks), F32),
                pltpu.VMEM((3, n, 4 * toks, d), BF16),
                pltpu.VMEM((3, n, 2, toks), F32),
                pltpu.VMEM((2, n, 3 * toks, d), BF16),
                pltpu.VMEM((3, n, 3 * toks, d), BF16),
                pltpu.VMEM((3, toks, n, d), BF16),
                pltpu.VMEM((toks // 4 * n, d), F32),
                pltpu.VMEM((n, d, toks), BF16),
                pltpu.VMEM((n, d, toks), F32),
                pltpu.VMEM((n, toks, d), F32),
                pltpu.VMEM((n, toks, d), F32),
                dma((n,)), dma((2, n)), dma((n,)), dma((2, n)), dma((n,)), dma((2, n)),
                dma((5,)), dma, dma((3,)),
            ],
            compiler_params=pltpu.CompilerParams(
                collective_id=0, has_side_effects=True, vmem_limit_bytes=67_043_328),
        )(q[0], k[0], v[0], o[0], do[0], lse[0])
        return dq[None], dk[None], dv[None]

    return jax.shard_map(local, mesh=mesh, in_specs=(spec, spec, spec, spec, lspec, spec),
                         out_specs=(spec, spec, spec), check_vma=False)
```

```python
import functools

import jax
import jax.numpy as jnp
from jax import lax
from jax.experimental import pallas as pl
from jax.experimental.pallas import tpu as pltpu
from jax.sharding import PartitionSpec as P

F32 = jnp.float32
BF16 = jnp.bfloat16
MESH = pl.DeviceIdType.MESH


NT = (((1,), (1,)), ((), ()))
NN = (((1,), (0,)), ((), ()))


def _dot(a, b, dims):
    return lax.dot_general(a, b, dims, preferred_element_type=F32)


def _kernel(n, toks, heads, q_ref, k_ref, v_ref, o_ref, do_ref, lse_ref, dq_ref, dk_ref, dv_ref, *rest):
    last_refs, rest = rest[:n], rest[n:]
    (raw, raw_lse, snd, snd_st, rcv, rcv_st, osnd, orcv, ostage, tmp, kt, dqt, dka, dva,
            isend, irecv, ssend, srecv, osend, orecv, ldsem, lsesem, stsem, lastsem) = rest
    half = toks // 2
    d = q_ref.shape[-1]
    scale = d ** -0.5
    chunks = heads // n
    me = lax.axis_index('cp')
    row = lax.axis_index('data')

    def peer(r):
        p = me
        if r & 1:
            p = p + 1 - 2 * lax.rem(me, 2)
        if r & 2:
            p = p + 2 - 4 * lax.rem(me // 2, 2)
        if r & 4:
            p = p + 4 - 8 * lax.rem(me // 4, 2)
        return p

    srcs = (q_ref, k_ref, v_ref, do_ref, o_ref)
    dsts = (dq_ref, dk_ref, dv_ref)

    def loads(c):
        h = pl.ds(pl.multiple_of(c * n, n), n)
        out = [pltpu.make_async_copy(x.at[:, h, :], raw.at[a], ldsem.at[a]) for a, x in enumerate(srcs)]
        out.append(pltpu.make_async_copy(lse_ref.at[h, :], raw_lse, lsesem))
        return out

    def stores(c):
        h = pl.ds(pl.multiple_of(c * n, n), n)
        return [pltpu.make_async_copy(ostage.at[a], x.at[:, h, :], stsem.at[a]) for a, x in enumerate(dsts)]

    def remote(src, dst, ssem, rsem, p):
        return pltpu.make_async_remote_copy(src_ref=src, dst_ref=dst, send_sem=ssem, recv_sem=rsem,
                                            device_id=(row, p), device_id_type=MESH)

    def in_copies(s, r, at):
        p = peer(r)
        a, b, par = lax.rem(s, 2), lax.rem(s, 3), lax.rem(s, 2)
        return (remote(snd.at[a, p], rcv.at[b, at], isend.at[r], irecv.at[par, r], p),
                remote(snd_st.at[a, p], rcv_st.at[b, at], ssend.at[r], srecv.at[par, r], p))

    def out_copies(c, r, at):
        p = peer(r)
        a, b, par = lax.rem(c, 2), lax.rem(c, 3), lax.rem(c, 2)
        return (remote(osnd.at[a, p], orcv.at[b, at], osend.at[r], orecv.at[par, r], p),)

    def prepare(c):
        a_slot = lax.rem(c, 2)
        part = toks // 4

        def tensor(a, _):
            def piece(i, _):
                rows = pl.ds(pl.multiple_of(i * part, part), part)
                x = raw[a, rows].astype(F32).reshape(part * n, d)
                tmp[pl.ds(0, part * n), :] = x
                for h in range(n):
                    snd[a_slot, h, pl.ds(pl.multiple_of(a * toks + i * part, part), part), :] = (
                        tmp[pl.ds(h, part, stride=n), :].astype(BF16))
                return 0
            return lax.fori_loop(0, 4, piece, 0)
        lax.fori_loop(0, 4, tensor, 0)

        def stat(i, _):
            rows = pl.ds(pl.multiple_of(i * part, part), part)
            x = raw[3, rows].astype(F32) * raw[4, rows].astype(F32)
            tmp[pl.ds(0, part * n), :] = x.reshape(part * n, d)
            for h in range(n):
                y = tmp[pl.ds(h, part, stride=n), :]
                snd_st[a_slot, h, 1:2, pl.ds(pl.multiple_of(i * part, part), part)] = (
                    jnp.sum(y.T, axis=0, keepdims=True))
            return 0
        lax.fori_loop(0, 4, stat, 0)
        for h in range(n):
            snd_st[a_slot, h, 0:1, :] = raw_lse[h:h + 1, :]

    def finalize(c):
        b_slot = lax.rem(c, 3)
        part = toks // 4

        def tensor(a, _):
            def piece(i, _):
                rows = pl.ds(pl.multiple_of(i * part, part), part)
                for h in range(n):
                    tmp[pl.ds(h, part, stride=n), :] = (
                        orcv[b_slot, h, pl.ds(pl.multiple_of(a * toks + i * part, part), part), :].astype(F32))
                ostage[a, rows] = tmp[pl.ds(0, part * n), :].reshape(part, n, d).astype(BF16)
                return 0
            return lax.fori_loop(0, 4, piece, 0)
        lax.fori_loop(0, 3, tensor, 0)

    def tile(b, i, q0, qn, j, k0, kn, mask):
        q = rcv[b, i, q0:q0 + qn, :]
        k = rcv[b, j, toks + k0:toks + k0 + kn, :]
        v = rcv[b, j, 2 * toks + k0:2 * toks + k0 + kn, :]
        do = rcv[b, i, 3 * toks + q0:3 * toks + q0 + qn, :]
        lse = rcv_st[b, i, 0:1, q0:q0 + qn]
        delta = rcv_st[b, i, 1:2, q0:q0 + qn]
        p = jnp.exp(_dot(k, q, NT) * scale - lse)
        if mask is not None:
            p = jnp.where(mask, p, 0.0)
        dp = _dot(v, do, NT)
        ds = (p * (dp - delta)).astype(BF16)
        dva[j, k0:k0 + kn, :] += _dot(p.astype(BF16), do, NN)
        dka[j, k0:k0 + kn, :] += _dot(ds, q, NN)
        dqt[i, :, q0:q0 + qn] += _dot(kt[j, :, k0:k0 + kn], ds, NN)

    def begin(c):
        b = lax.rem(c, 3)

        def clear(j, _):
            kt[j] = rcv[b, j, toks:2 * toks, :].T
            dqt[j] = jnp.zeros((d, toks), F32)
            dka[j] = jnp.zeros((toks, d), F32)
            dva[j] = jnp.zeros((toks, d), F32)
            return 0
        lax.fori_loop(0, n, clear, 0)

    def compute(c, lo, hi):
        b = lax.rem(c, 3)
        tri = (lax.broadcasted_iota(jnp.int32, (half, half), 0)
               <= lax.broadcasted_iota(jnp.int32, (half, half), 1))

        def keys(j, _):
            tile(b, j, 0, half, j, 0, half, tri)
            tile(b, j, half, half, j, 0, half, None)
            tile(b, j, half, half, j, half, half, tri)

            def lower(i, _):
                tile(b, i, half, half, j, 0, toks, None)
                return 0
            lax.fori_loop(0, j, lower, 0)

            def higher(i, _):
                tile(b, i, 0, toks, j, 0, half, None)
                return 0
            lax.fori_loop(j + 1, n, higher, 0)
            return 0
        lax.fori_loop(lo, hi, keys, 0)

    def finish(c):
        oslot = lax.rem(c, 2)

        def block(i, _):
            osnd[oslot, i, 0:toks, :] = (dqt[i].T * scale).astype(BF16)
            osnd[oslot, i, toks:2 * toks, :] = (dka[i] * scale).astype(BF16)
            osnd[oslot, i, 2 * toks:3 * toks, :] = dva[i].astype(BF16)
            return 0
        lax.fori_loop(0, n, block, 0)

    for x in loads(0):
        x.start()
    barrier = pltpu.get_barrier_semaphore()
    for r in range(1, n):
        pl.semaphore_signal(barrier, inc=1, device_id=(row, peer(r)), device_id_type=MESH)
    for x in loads(0):
        x.wait()
    prepare(0)
    for x in loads(1):
        x.start()
    pl.semaphore_wait(barrier, n - 1)

    order = (2, 4, 3, 5, 1, 6, 7)

    def begin_in(s):
        for r in order:
            for x in in_copies(s, r, me):
                x.start()
        a, b = lax.rem(s, 2), lax.rem(s, 3)
        rcv[b, me] = snd[a, me]
        rcv_st[b, me] = snd_st[a, me]

    def end_in(s):
        for r in range(1, n):
            for x in in_copies(s, r, me):
                x.wait_send()
            for x in in_copies(s, r, peer(r)):
                x.wait_recv()

    def begin_out(c):
        for r in order:
            for x in out_copies(c, r, me):
                x.start()
        a, b = lax.rem(c, 2), lax.rem(c, 3)
        orcv[b, me] = osnd[a, me]

    def end_out(c):
        for r in range(1, n):
            for x in out_copies(c, r, me):
                x.wait_send()
            for x in out_copies(c, r, peer(r)):
                x.wait_recv()

    def step(s, _):
        computes = (s >= 1) & (s < chunks + 1)

        @pl.when(computes)
        def _():
            end_in(s - 1)

        @pl.when(s < chunks)
        def _():
            begin_in(s)

        @pl.when(s >= 4)
        def _():
            for x in stores(s - 4):
                x.start()

        @pl.when(computes)
        def _():
            begin(s - 1)
            compute(s - 1, 0, n // 2)

        @pl.when(s >= 3)
        def _():
            end_out(s - 3)

        @pl.when((s >= 2) & (s < chunks + 1))
        def _():
            begin_out(s - 2)

        @pl.when(computes)
        def _():
            compute(s - 1, n // 2, n)
            finish(s - 1)

        @pl.when(s + 1 < chunks)
        def _():
            for x in loads(s + 1):
                x.wait()
            prepare(s + 1)

        @pl.when(s + 2 < chunks)
        def _():
            for x in loads(s + 2):
                x.start()

        @pl.when(s >= 4)
        def _():
            for x in stores(s - 4):
                x.wait()

        @pl.when(s >= 3)
        def _():
            finalize(s - 3)
        return 0

    def last():
        return [pltpu.make_async_copy(osnd.at[(chunks - 1) % 2, peer(r)], x, lastsem.at[r])
                for r, x in enumerate(last_refs)]

    lax.fori_loop(0, chunks + 1, step, 0)
    for x in last():
        x.start()
    for x in stores(chunks - 3):
        x.start()
    end_out(chunks - 2)
    for x in stores(chunks - 3):
        x.wait()
    finalize(chunks - 2)
    for x in stores(chunks - 2):
        x.start()
    for x in stores(chunks - 2) + last():
        x.wait()


def _move_kernel(rows, *refs):
    srcs, dsts, (buf, rsem, wsem) = refs[:3], refs[3:6], refs[6:]
    slots = buf.shape[0]
    heads = srcs[0].shape[1]
    blocks = [(a, i) for i in range(srcs[0].shape[0] // rows) for a in range(3)]

    def read(t):
        a, i = blocks[t]
        return pltpu.make_async_copy(srcs[a].at[i * rows:(i + 1) * rows], buf.at[t % slots], rsem.at[t % slots])

    def write(t):
        a, i = blocks[t]
        return pltpu.make_async_copy(buf.at[t % slots], dsts[a].at[i * rows:(i + 1) * rows, 0:heads, :],
                                     wsem.at[t % slots])

    ahead = slots // 2
    for t in range(len(blocks) + ahead):
        if t < len(blocks):
            if t >= slots:
                write(t - slots).wait()
            read(t).start()
        if t >= ahead:
            read(t - ahead).wait()
            write(t - ahead).start()
    for t in range(max(0, len(blocks) - slots), len(blocks)):
        write(t).wait()


def _last_kernel(n, toks, *refs):
    parts, rest = refs[:n], refs[n + 3:]
    dsts, (buf, stage, tmp, rsem, wsem) = rest[:3], rest[3:]
    d = stage.shape[-1]
    heads = dsts[0].shape[1]
    me = lax.axis_index('cp')

    def peer(r):
        p = me
        for bit in (1, 2, 4):
            if r & bit:
                p = p + bit - 2 * bit * lax.rem(me // bit, 2)
        return p

    reads = [pltpu.make_async_copy(x, buf.at[peer(r)], rsem.at[r]) for r, x in enumerate(parts)]
    for x in reads:
        x.start()
    for x in reads:
        x.wait()
    piece = tmp.shape[0] // n
    writes = []
    for a in range(3):
        def block(i, _):
            for h in range(n):
                tmp[pl.ds(h, piece, stride=n), :] = (
                    buf[h, pl.ds(pl.multiple_of(a * toks + i * piece, piece), piece), :].astype(F32))
            stage[a, pl.ds(pl.multiple_of(i * piece, piece), piece)] = (
                tmp[...].reshape(piece, n, d).astype(BF16))
            return 0
        lax.fori_loop(0, toks // piece, block, 0)
        writes.append(pltpu.make_async_copy(stage.at[a], dsts[a].at[:, heads - n:heads, :], wsem.at[a]))
        writes[-1].start()
    for x in writes:
        x.wait()


def solution(mesh):
    n = mesh.shape['cp']
    spec = P('data', 'cp', None, None)
    lspec = P('data', None, 'cp')

    def local(q, k, v, o, lse, do):
        _, toks, heads, d = q.shape
        out = jax.ShapeDtypeStruct((toks, heads, d), BF16)
        early = jax.ShapeDtypeStruct((toks, heads - n, d), BF16)
        part = jax.ShapeDtypeStruct((3 * toks, d), BF16)
        any_ = pl.BlockSpec(memory_space=pl.ANY)
        dma = pltpu.SemaphoreType.DMA
        res = pl.pallas_call(
            functools.partial(_kernel, n, toks, heads),
            out_shape=(early,) * 3 + (part,) * n,
            in_specs=[any_] * 6,
            out_specs=(any_,) * (3 + n),
            scratch_shapes=[
                pltpu.VMEM((5, toks, n, d), BF16),
                pltpu.VMEM((n, toks), F32),
                pltpu.VMEM((2, n, 4 * toks, d), BF16),
                pltpu.VMEM((2, n, 2, toks), F32),
                pltpu.VMEM((3, n, 4 * toks, d), BF16),
                pltpu.VMEM((3, n, 2, toks), F32),
                pltpu.VMEM((2, n, 3 * toks, d), BF16),
                pltpu.VMEM((3, n, 3 * toks, d), BF16),
                pltpu.VMEM((3, toks, n, d), BF16),
                pltpu.VMEM((toks // 4 * n, d), F32),
                pltpu.VMEM((n, d, toks), BF16),
                pltpu.VMEM((n, d, toks), F32),
                pltpu.VMEM((n, toks, d), F32),
                pltpu.VMEM((n, toks, d), F32),
                dma((n,)), dma((2, n)), dma((n,)), dma((2, n)), dma((n,)), dma((2, n)),
                dma((5,)), dma, dma((3,)), dma((n,)),
            ],
            compiler_params=pltpu.CompilerParams(
                collective_id=0, has_side_effects=True, vmem_limit_bytes=67_043_328),
        )(q[0], k[0], v[0], o[0], do[0], lse[0])
        moved = 2 * 3 * toks * (heads - n) * d * 2
        rows, slots = 32, 16
        dq, dk, dv = pl.pallas_call(
            functools.partial(_move_kernel, rows),
            out_shape=(out, out, out),
            in_specs=[any_] * 3,
            out_specs=(any_,) * 3,
            scratch_shapes=[pltpu.VMEM((slots, rows, heads - n, d), BF16), dma((slots,)), dma((slots,))],
            cost_estimate=pl.CostEstimate(flops=0, bytes_accessed=moved, transcendentals=0),
        )(*res[:3])
        parts = [res[3]] + [lax.ppermute(res[3 + r], 'cp', [(j, j ^ r) for j in range(n)]) for r in range(1, n)]
        dq, dk, dv = pl.pallas_call(
            functools.partial(_last_kernel, n, toks),
            out_shape=(out, out, out),
            in_specs=[any_] * (n + 3),
            out_specs=(any_,) * 3,
            scratch_shapes=[
                pltpu.VMEM((n, 3 * toks, d), BF16), pltpu.VMEM((3, toks, n, d), BF16),
                pltpu.VMEM((toks // 4 * n, d), F32), dma((n,)), dma((3,)),
            ],
            input_output_aliases={n: 0, n + 1: 1, n + 2: 2},
            cost_estimate=pl.CostEstimate(flops=0, bytes_accessed=12 * toks * n * d, transcendentals=0),
        )(*parts, dq, dk, dv)
        return dq[None], dk[None], dv[None]

    return jax.shard_map(local, mesh=mesh, in_specs=(spec, spec, spec, spec, lspec, spec),
                         out_specs=(spec, spec, spec), check_vma=False)
```

```python
import functools

import jax
import jax.numpy as jnp
from jax import lax
from jax.experimental import pallas as pl
from jax.experimental.pallas import tpu as pltpu
from jax.sharding import PartitionSpec as P

F32 = jnp.float32
BF16 = jnp.bfloat16
MESH = pl.DeviceIdType.MESH


ORDER = (0, 2, 4, 3, 5, 6, 7, 1)

NT = (((1,), (1,)), ((), ()))
NN = (((1,), (0,)), ((), ()))


def _dot(a, b, dims):
    return lax.dot_general(a, b, dims, preferred_element_type=F32)


def _kernel(n, toks, heads, q_ref, k_ref, v_ref, o_ref, do_ref, lse_ref, dq_ref, dk_ref, dv_ref, *rest):
    near_ref, last_refs, rest = rest[0], rest[1:n + 1], rest[n + 1:]
    (raw, raw_lse, snd, snd_st, rcv, rcv_st, osnd, orcv, ostage, tmp, kt, dqt, dka, dva,
            isend, irecv, ssend, srecv, osend, orecv, ldsem, lsesem, stsem, lastsem, nearsem) = rest
    half = toks // 2
    d = q_ref.shape[-1]
    scale = d ** -0.5
    chunks = heads // n
    me = lax.axis_index('cp')
    row = lax.axis_index('data')

    def peer(r):
        p = me
        if r & 1:
            p = p + 1 - 2 * lax.rem(me, 2)
        if r & 2:
            p = p + 2 - 4 * lax.rem(me // 2, 2)
        if r & 4:
            p = p + 4 - 8 * lax.rem(me // 4, 2)
        return p

    srcs = (q_ref, k_ref, v_ref, do_ref, o_ref)
    dsts = (dq_ref, dk_ref, dv_ref)

    def loads(c):
        h = pl.ds(pl.multiple_of(c * n, n), n)
        out = [pltpu.make_async_copy(x.at[:, h, :], raw.at[a], ldsem.at[a]) for a, x in enumerate(srcs)]
        out.append(pltpu.make_async_copy(lse_ref.at[h, :], raw_lse, lsesem))
        return out

    def stores(c):
        h = pl.ds(pl.multiple_of(c * n, n), n)
        return [pltpu.make_async_copy(ostage.at[a], x.at[:, h, :], stsem.at[a]) for a, x in enumerate(dsts)]

    def remote(src, dst, ssem, rsem, p):
        return pltpu.make_async_remote_copy(src_ref=src, dst_ref=dst, send_sem=ssem, recv_sem=rsem,
                                            device_id=(row, p), device_id_type=MESH)

    def in_tokens(s, r, at, rows=slice(None)):
        p = peer(r)
        a, b, par = lax.rem(s, 2), lax.rem(s, 3), lax.rem(s, 2)
        return remote(snd.at[a, p, rows], rcv.at[b, at, rows], isend.at[par, r], irecv.at[b, r], p)

    def in_stats(s, r, at):
        p = peer(r)
        a, b, par = lax.rem(s, 2), lax.rem(s, 3), lax.rem(s, 2)
        return remote(snd_st.at[a, p], rcv_st.at[b, at], ssend.at[par, r], srecv.at[b, r], p)

    def out_copy(c, r, at):
        p = peer(r)
        a, b, par = lax.rem(c, 2), lax.rem(c, 3), lax.rem(c, 2)
        return remote(osnd.at[a, p], orcv.at[b, at], osend.at[par, r], orecv.at[b, r], p)

    def near_copy(r, at):
        c = chunks - 2
        p = peer(r)
        return remote(osnd.at[c % 2, p], near_ref.at[at], osend.at[c % 2, r], orecv.at[c % 3, r], p)

    part = toks // 4

    def split(c, a):
        a_slot = lax.rem(c, 2)

        def piece(i, _):
            rows = pl.ds(pl.multiple_of(i * part, part), part)
            x = raw[a, rows].astype(F32).reshape(part * n, d)
            tmp[pl.ds(0, part * n), :] = x
            for h in range(n):
                snd[a_slot, h, pl.ds(pl.multiple_of(a * toks + i * part, part), part), :] = (
                    tmp[pl.ds(h, part, stride=n), :].astype(BF16))
            return 0
        lax.fori_loop(0, 4, piece, 0)

    def stats(c):
        a_slot = lax.rem(c, 2)
        for h in range(n):
            snd_st[a_slot, h, 0:1, :] = raw_lse[h:h + 1, :]

        def stat(i, _):
            rows = pl.ds(pl.multiple_of(i * part, part), part)
            x = raw[3, rows].astype(F32) * raw[4, rows].astype(F32)
            tmp[pl.ds(0, part * n), :] = x.reshape(part * n, d)
            for h in range(n):
                y = tmp[pl.ds(h, part, stride=n), :]
                snd_st[a_slot, h, 1:2, pl.ds(pl.multiple_of(i * part, part), part)] = (
                    jnp.sum(y.T, axis=0, keepdims=True))
            return 0
        lax.fori_loop(0, 4, stat, 0)

    def prepare(c):
        def tensor(a, _):
            split(c, a)
            return 0
        lax.fori_loop(0, 4, tensor, 0)
        stats(c)

    def finalize(c):
        b_slot = lax.rem(c, 3)

        def tensor(a, _):
            def piece(i, _):
                rows = pl.ds(pl.multiple_of(i * part, part), part)
                for h in range(n):
                    tmp[pl.ds(h, part, stride=n), :] = (
                        orcv[b_slot, h, pl.ds(pl.multiple_of(a * toks + i * part, part), part), :].astype(F32))
                ostage[a, rows] = tmp[pl.ds(0, part * n), :].reshape(part, n, d).astype(BF16)
                return 0
            return lax.fori_loop(0, 4, piece, 0)
        lax.fori_loop(0, 3, tensor, 0)

    def tile(b, i, q0, qn, j, k0, kn, mask):
        q = rcv[b, i, q0:q0 + qn, :]
        k = rcv[b, j, toks + k0:toks + k0 + kn, :]
        v = rcv[b, j, 2 * toks + k0:2 * toks + k0 + kn, :]
        do = rcv[b, i, 3 * toks + q0:3 * toks + q0 + qn, :]
        lse = rcv_st[b, i, 0:1, q0:q0 + qn]
        delta = rcv_st[b, i, 1:2, q0:q0 + qn]
        p = jnp.exp(_dot(k, q, NT) * scale - lse)
        if mask is not None:
            p = jnp.where(mask, p, 0.0)
        dp = _dot(v, do, NT)
        ds = (p * (dp - delta)).astype(BF16)
        dva[j, k0:k0 + kn, :] += _dot(p.astype(BF16), do, NN)
        dka[j, k0:k0 + kn, :] += _dot(ds, q, NN)
        dqt[i, :, q0:q0 + qn] += _dot(kt[j, :, k0:k0 + kn], ds, NN)

    def begin(c):
        b = lax.rem(c, 3)

        def clear(j, _):
            kt[j] = rcv[b, j, toks:2 * toks, :].T
            dqt[j] = jnp.zeros((d, toks), F32)
            dka[j] = jnp.zeros((toks, d), F32)
            dva[j] = jnp.zeros((toks, d), F32)
            return 0
        lax.fori_loop(0, n, clear, 0)

    def compute(c, lo, hi):
        b = lax.rem(c, 3)
        tri = (lax.broadcasted_iota(jnp.int32, (half, half), 0)
               <= lax.broadcasted_iota(jnp.int32, (half, half), 1))

        def keys(j, _):
            tile(b, j, 0, half, j, 0, half, tri)
            tile(b, j, half, half, j, 0, half, None)
            tile(b, j, half, half, j, half, half, tri)

            def lower(i, _):
                tile(b, i, half, half, j, 0, toks, None)
                return 0
            lax.fori_loop(0, j, lower, 0)

            def higher(i, _):
                tile(b, i, 0, toks, j, 0, half, None)
                return 0
            lax.fori_loop(j + 1, n, higher, 0)
            return 0
        lax.fori_loop(lo, hi, keys, 0)

    def finish(c):
        oslot = lax.rem(c, 2)

        def block(i, _):
            osnd[oslot, i, 0:toks, :] = (dqt[i].T * scale).astype(BF16)
            osnd[oslot, i, toks:2 * toks, :] = (dka[i] * scale).astype(BF16)
            osnd[oslot, i, 2 * toks:3 * toks, :] = dva[i].astype(BF16)
            return 0
        lax.fori_loop(0, n, block, 0)

    order = (2, 4, 3, 5, 1, 6, 7)

    def own(s):
        a, b = lax.rem(s, 2), lax.rem(s, 3)
        rcv[b, me] = snd[a, me]
        rcv_st[b, me] = snd_st[a, me]

    def begin_in(s):
        for r in order:
            in_tokens(s, r, me).start()
        own(s)
        for r in order:
            in_stats(s, r, me).start()

    def end_in(s):
        for r in range(1, n):
            in_tokens(s, r, me).wait_send()
            in_stats(s, r, me).wait_send()
            in_tokens(s, r, peer(r)).wait_recv()
            in_stats(s, r, peer(r)).wait_recv()

    def begin_out(c):
        for r in order:
            out_copy(c, r, me).start()
        a, b = lax.rem(c, 2), lax.rem(c, 3)
        orcv[b, me] = osnd[a, me]

    def end_out(c):
        for r in range(1, n):
            out_copy(c, r, me).wait_send()
            out_copy(c, r, peer(r)).wait_recv()

    first = loads(0)
    for x in first:
        x.start()
    barrier = pltpu.get_barrier_semaphore()
    for r in range(1, n):
        pl.semaphore_signal(barrier, inc=1, device_id=(row, peer(r)), device_id_type=MESH)
    for a in range(5):
        first[a].wait()
        if a < 4:
            split(0, a)
        else:
            first[5].wait()
            stats(0)
        if a == 1:
            pl.semaphore_wait(barrier, n - 1)
        if a:
            for r in order:
                in_tokens(0, r, me, pl.ds((a - 1) * toks, toks)).start()
    own(0)
    for r in order:
        in_stats(0, r, me).start()
    for x in loads(1):
        x.start()

    def step(s, _):
        computes = s >= 1

        @pl.when(computes)
        def _():
            end_in(s - 1)

        @pl.when((s >= 3) & (s < chunks))
        def _():
            begin_in(s)

        @pl.when(s == chunks)
        def _():
            for r in order:
                near_copy(r, me).start()
            pltpu.make_async_copy(osnd.at[(chunks - 2) % 2, me], near_ref.at[me], nearsem).start()

        @pl.when(s >= 4)
        def _():
            for x in stores(s - 4):
                x.start()

        @pl.when(computes)
        def _():
            begin(s - 1)
            compute(s - 1, 0, n // 2)

        @pl.when(s >= 3)
        def _():
            end_out(s - 3)

        @pl.when((s >= 2) & (s < chunks))
        def _():
            begin_out(s - 2)

        @pl.when(computes)
        def _():
            compute(s - 1, n // 2, n)
            finish(s - 1)

        @pl.when(s + 1 < chunks)
        def _():
            for x in loads(s + 1):
                x.wait()
            prepare(s + 1)

        @pl.when(s < 2)
        def _():
            begin_in(s + 1)

        @pl.when(s + 2 < chunks)
        def _():
            for x in loads(s + 2):
                x.start()

        @pl.when(s >= 4)
        def _():
            for x in stores(s - 4):
                x.wait()

        @pl.when(s >= 3)
        def _():
            finalize(s - 3)
        return 0

    lax.fori_loop(0, chunks + 1, step, 0)

    tail = [pltpu.make_async_copy(osnd.at[(chunks - 1) % 2, peer(r)], x, lastsem.at[r])
            for r, x in zip(ORDER, last_refs)] + stores(chunks - 3)
    for x in tail:
        x.start()
    pltpu.make_async_copy(osnd.at[(chunks - 2) % 2, me], near_ref.at[me], nearsem).wait()
    for x in tail:
        x.wait()
    for r in range(1, n):
        near_copy(r, me).wait_send()
        near_copy(r, peer(r)).wait_recv()


def _merge(n, toks, at, dsts, buf, stage, tmp, wsem):
    d = stage.shape[-1]
    piece = tmp.shape[0] // n
    writes = []
    for a in range(3):
        def block(i, _):
            for h in range(n):
                tmp[pl.ds(h, piece, stride=n), :] = (
                    buf[h, pl.ds(pl.multiple_of(a * toks + i * piece, piece), piece), :].astype(F32))
            stage[a, pl.ds(pl.multiple_of(i * piece, piece), piece)] = (
                tmp[...].reshape(piece, n, d).astype(BF16))
            return 0
        lax.fori_loop(0, toks // piece, block, 0)
        writes.append(pltpu.make_async_copy(stage.at[a], dsts[a].at[:, at:at + n, :], wsem.at[a]))
        writes[-1].start()
    return writes


def _move_kernel(n, toks, rows, *refs):
    srcs, near, dsts, (buf, rsem, wsem, nbuf, stage, tmp, nsem, msem) = refs[:3], refs[3], refs[4:7], refs[7:]
    other = pltpu.make_async_copy(near, nbuf, nsem)
    other.start()
    slots = buf.shape[0]
    heads = srcs[0].shape[1]
    blocks = [(a, i) for i in range(srcs[0].shape[0] // rows) for a in range(3)]

    def read(t):
        a, i = blocks[t]
        return pltpu.make_async_copy(srcs[a].at[i * rows:(i + 1) * rows], buf.at[t % slots], rsem.at[t % slots])

    def write(t):
        a, i = blocks[t]
        return pltpu.make_async_copy(buf.at[t % slots], dsts[a].at[i * rows:(i + 1) * rows, 0:heads, :],
                                     wsem.at[t % slots])

    ahead = slots // 2
    for t in range(len(blocks) + ahead):
        if t < len(blocks):
            if t >= slots:
                write(t - slots).wait()
            read(t).start()
        if t >= ahead:
            read(t - ahead).wait()
            write(t - ahead).start()
        if t == len(blocks) // 2:
            other.wait()
            merged = _merge(n, toks, heads, dsts, nbuf, stage, tmp, msem)
    for t in range(max(0, len(blocks) - slots), len(blocks)):
        write(t).wait()
    for x in merged:
        x.wait()


def _last_kernel(n, toks, *refs):
    parts, rest = refs[:n], refs[n + 3:]
    dsts, (buf, stage, tmp, rsem, wsem) = rest[:3], rest[3:]
    heads = dsts[0].shape[1]
    me = lax.axis_index('cp')

    def peer(r):
        p = me
        for bit in (1, 2, 4):
            if r & bit:
                p = p + bit - 2 * bit * lax.rem(me // bit, 2)
        return p

    reads = [pltpu.make_async_copy(x, buf.at[peer(r)], rsem.at[r]) for r, x in zip(ORDER, parts)]
    for x in reads:
        x.start()
    for x in reads:
        x.wait()
    for x in _merge(n, toks, heads - n, dsts, buf, stage, tmp, wsem):
        x.wait()


def solution(mesh):
    n = mesh.shape['cp']
    spec = P('data', 'cp', None, None)
    lspec = P('data', None, 'cp')

    def local(q, k, v, o, lse, do):
        _, toks, heads, d = q.shape
        out = jax.ShapeDtypeStruct((toks, heads, d), BF16)
        early = jax.ShapeDtypeStruct((toks, heads - 2 * n, d), BF16)
        near = jax.ShapeDtypeStruct((n, 3 * toks, d), BF16)
        part = jax.ShapeDtypeStruct((3 * toks, d), BF16)
        any_ = pl.BlockSpec(memory_space=pl.ANY)
        dma = pltpu.SemaphoreType.DMA
        res = pl.pallas_call(
            functools.partial(_kernel, n, toks, heads),
            out_shape=(early,) * 3 + (near,) + (part,) * n,
            in_specs=[any_] * 6,
            out_specs=(any_,) * (4 + n),
            scratch_shapes=[
                pltpu.VMEM((5, toks, n, d), BF16),
                pltpu.VMEM((n, toks), F32),
                pltpu.VMEM((2, n, 4 * toks, d), BF16),
                pltpu.VMEM((2, n, 2, toks), F32),
                pltpu.VMEM((3, n, 4 * toks, d), BF16),
                pltpu.VMEM((3, n, 2, toks), F32),
                pltpu.VMEM((2, n, 3 * toks, d), BF16),
                pltpu.VMEM((3, n, 3 * toks, d), BF16),
                pltpu.VMEM((3, toks, n, d), BF16),
                pltpu.VMEM((toks // 4 * n, d), F32),
                pltpu.VMEM((n, d, toks), BF16),
                pltpu.VMEM((n, d, toks), F32),
                pltpu.VMEM((n, toks, d), F32),
                pltpu.VMEM((n, toks, d), F32),
                dma((2, n)), dma((3, n)), dma((2, n)), dma((3, n)), dma((2, n)), dma((3, n)),
                dma((5,)), dma, dma((3,)), dma((n,)), dma,
            ],
            compiler_params=pltpu.CompilerParams(
                collective_id=0, has_side_effects=True, vmem_limit_bytes=67_043_328),
        )(q[0], k[0], v[0], o[0], do[0], lse[0])
        moved = 2 * 3 * toks * (heads - n) * d * 2
        rows, slots = 32, 16
        dq, dk, dv = pl.pallas_call(
            functools.partial(_move_kernel, n, toks, rows),
            out_shape=(out, out, out),
            in_specs=[any_] * 4,
            out_specs=(any_,) * 3,
            scratch_shapes=[
                pltpu.VMEM((slots, rows, heads - 2 * n, d), BF16), dma((slots,)), dma((slots,)),
                pltpu.VMEM((n, 3 * toks, d), BF16), pltpu.VMEM((3, toks, n, d), BF16),
                pltpu.VMEM((toks // 4 * n, d), F32), dma, dma((3,)),
            ],
            cost_estimate=pl.CostEstimate(flops=0, bytes_accessed=moved, transcendentals=0),
        )(*res[:4])
        parts = [res[4]] + [lax.ppermute(x, 'cp', [(j, j ^ r) for j in range(n)])
                            for r, x in zip(ORDER[1:], res[5:])]
        dq, dk, dv = pl.pallas_call(
            functools.partial(_last_kernel, n, toks),
            out_shape=(out, out, out),
            in_specs=[any_] * (n + 3),
            out_specs=(any_,) * 3,
            scratch_shapes=[
                pltpu.VMEM((n, 3 * toks, d), BF16), pltpu.VMEM((3, toks, n, d), BF16),
                pltpu.VMEM((toks // 4 * n, d), F32), dma((n,)), dma((3,)),
            ],
            input_output_aliases={n: 0, n + 1: 1, n + 2: 2},
            cost_estimate=pl.CostEstimate(flops=0, bytes_accessed=12 * toks * n * d, transcendentals=0),
        )(*parts, dq, dk, dv)
        return dq[None], dk[None], dv[None]

    return jax.shard_map(local, mesh=mesh, in_specs=(spec, spec, spec, spec, lspec, spec),
                         out_specs=(spec, spec, spec), check_vma=False)
```

```python
import functools

import jax
import jax.numpy as jnp
from jax import lax
from jax.experimental import pallas as pl
from jax.experimental.pallas import tpu as pltpu
from jax.sharding import PartitionSpec as P

F32 = jnp.float32
BF16 = jnp.bfloat16
MESH = pl.DeviceIdType.MESH


ORDER = (0, 2, 4, 3, 5, 6, 7, 1)

NT = (((1,), (1,)), ((), ()))
NN = (((1,), (0,)), ((), ()))


def _dot(a, b, dims):
    return lax.dot_general(a, b, dims, preferred_element_type=F32)


def _kernel(n, toks, heads, q_ref, k_ref, v_ref, o_ref, do_ref, lse_ref, dq_ref, dk_ref, dv_ref, *rest):
    near_ref, last_refs, rest = rest[0], rest[1:n + 1], rest[n + 1:]
    (raw, raw_lse, snd, snd_st, rcv, rcv_st, osnd, orcv, ostage, tmp, kt, dqt, dka, dva,
            isend, irecv, ssend, srecv, osend, orecv, ldsem, lsesem, stsem, lastsem, nearsem) = rest
    half = toks // 2
    d = q_ref.shape[-1]
    scale = d ** -0.5
    chunks = heads // n
    me = lax.axis_index('cp')
    row = lax.axis_index('data')

    def peer(r):
        p = me
        if r & 1:
            p = p + 1 - 2 * lax.rem(me, 2)
        if r & 2:
            p = p + 2 - 4 * lax.rem(me // 2, 2)
        if r & 4:
            p = p + 4 - 8 * lax.rem(me // 4, 2)
        return p

    srcs = (q_ref, k_ref, v_ref, do_ref, o_ref)
    dsts = (dq_ref, dk_ref, dv_ref)

    def loads(c):
        h = pl.ds(pl.multiple_of(c * n, n), n)
        out = [pltpu.make_async_copy(x.at[:, h, :], raw.at[a], ldsem.at[a]) for a, x in enumerate(srcs)]
        out.append(pltpu.make_async_copy(lse_ref.at[h, :], raw_lse, lsesem))
        return out

    def stores(c):
        h = pl.ds(pl.multiple_of(c * n, n), n)
        return [pltpu.make_async_copy(ostage.at[a], x.at[:, h, :], stsem.at[a]) for a, x in enumerate(dsts)]

    def remote(src, dst, ssem, rsem, p):
        return pltpu.make_async_remote_copy(src_ref=src, dst_ref=dst, send_sem=ssem, recv_sem=rsem,
                                            device_id=(row, p), device_id_type=MESH)

    def in_tokens(s, r, at, rows=slice(None)):
        p = peer(r)
        a, b, par = lax.rem(s, 2), lax.rem(s, 3), lax.rem(s, 2)
        return remote(snd.at[a, p, rows], rcv.at[b, at, rows], isend.at[par, r], irecv.at[b, r], p)

    def in_stats(s, r, at):
        p = peer(r)
        a, b, par = lax.rem(s, 2), lax.rem(s, 3), lax.rem(s, 2)
        return remote(snd_st.at[a, p], rcv_st.at[b, at], ssend.at[par, r], srecv.at[b, r], p)

    def out_copy(c, r, at):
        p = peer(r)
        a, b, par = lax.rem(c, 2), lax.rem(c, 3), lax.rem(c, 2)
        return remote(osnd.at[a, p], orcv.at[b, at], osend.at[par, r], orecv.at[b, r], p)

    def near_copy(r, at):
        c = chunks - 2
        p = peer(r)
        return remote(osnd.at[c % 2, p], near_ref.at[at], osend.at[c % 2, r], orecv.at[c % 3, r], p)

    part = toks // 4

    def split(c, a):
        a_slot = lax.rem(c, 2)

        def piece(i, _):
            rows = pl.ds(pl.multiple_of(i * part, part), part)
            x = raw[a, rows].astype(F32).reshape(part * n, d)
            tmp[pl.ds(0, part * n), :] = x
            for h in range(n):
                snd[a_slot, h, pl.ds(pl.multiple_of(a * toks + i * part, part), part), :] = (
                    tmp[pl.ds(h, part, stride=n), :].astype(BF16))
            return 0
        lax.fori_loop(0, 4, piece, 0)

    def stats(c):
        a_slot = lax.rem(c, 2)
        for h in range(n):
            snd_st[a_slot, h, 0:1, :] = raw_lse[h:h + 1, :]

        def stat(i, _):
            rows = pl.ds(pl.multiple_of(i * part, part), part)
            x = raw[3, rows].astype(F32) * raw[4, rows].astype(F32)
            tmp[pl.ds(0, part * n), :] = x.reshape(part * n, d)
            for h in range(n):
                y = tmp[pl.ds(h, part, stride=n), :]
                snd_st[a_slot, h, 1:2, pl.ds(pl.multiple_of(i * part, part), part)] = (
                    jnp.sum(y.T, axis=0, keepdims=True))
            return 0
        lax.fori_loop(0, 4, stat, 0)

    def prepare(c):
        def tensor(a, _):
            split(c, a)
            return 0
        lax.fori_loop(0, 4, tensor, 0)
        stats(c)

    def finalize(c):
        b_slot = lax.rem(c, 3)

        def tensor(a, _):
            def piece(i, _):
                rows = pl.ds(pl.multiple_of(i * part, part), part)
                for h in range(n):
                    tmp[pl.ds(h, part, stride=n), :] = (
                        orcv[b_slot, h, pl.ds(pl.multiple_of(a * toks + i * part, part), part), :].astype(F32))
                ostage[a, rows] = tmp[pl.ds(0, part * n), :].reshape(part, n, d).astype(BF16)
                return 0
            return lax.fori_loop(0, 4, piece, 0)
        lax.fori_loop(0, 3, tensor, 0)

    def tile(b, i, q0, qn, j, k0, kn, mask):
        q = rcv[b, i, q0:q0 + qn, :]
        k = rcv[b, j, toks + k0:toks + k0 + kn, :]
        v = rcv[b, j, 2 * toks + k0:2 * toks + k0 + kn, :]
        do = rcv[b, i, 3 * toks + q0:3 * toks + q0 + qn, :]
        lse = rcv_st[b, i, 0:1, q0:q0 + qn]
        delta = rcv_st[b, i, 1:2, q0:q0 + qn]
        p = jnp.exp(_dot(k, q, NT) * scale - lse)
        if mask is not None:
            p = jnp.where(mask, p, 0.0)
        dp = _dot(v, do, NT)
        ds = (p * (dp - delta)).astype(BF16)
        dva[j, k0:k0 + kn, :] += _dot(p.astype(BF16), do, NN)
        dka[j, k0:k0 + kn, :] += _dot(ds, q, NN)
        dqt[i, :, q0:q0 + qn] += _dot(kt[j, :, k0:k0 + kn], ds, NN)

    def begin(c):
        b = lax.rem(c, 3)

        def clear(j, _):
            kt[j] = rcv[b, j, toks:2 * toks, :].T
            dqt[j] = jnp.zeros((d, toks), F32)
            dka[j] = jnp.zeros((toks, d), F32)
            dva[j] = jnp.zeros((toks, d), F32)
            return 0
        lax.fori_loop(0, n, clear, 0)

    def compute(c, lo, hi):
        b = lax.rem(c, 3)
        tri = (lax.broadcasted_iota(jnp.int32, (half, half), 0)
               <= lax.broadcasted_iota(jnp.int32, (half, half), 1))

        def keys(j, _):
            tile(b, j, 0, half, j, 0, half, tri)
            tile(b, j, half, half, j, 0, half, None)
            tile(b, j, half, half, j, half, half, tri)

            def lower(i, _):
                tile(b, i, half, half, j, 0, toks, None)
                return 0
            lax.fori_loop(0, j, lower, 0)

            def higher(i, _):
                tile(b, i, 0, toks, j, 0, half, None)
                return 0
            lax.fori_loop(j + 1, n, higher, 0)
            return 0
        lax.fori_loop(lo, hi, keys, 0)

    def finish(c):
        oslot = lax.rem(c, 2)

        def block(i, _):
            osnd[oslot, i, 0:toks, :] = (dqt[i].T * scale).astype(BF16)
            osnd[oslot, i, toks:2 * toks, :] = (dka[i] * scale).astype(BF16)
            osnd[oslot, i, 2 * toks:3 * toks, :] = dva[i].astype(BF16)
            return 0
        lax.fori_loop(0, n, block, 0)

    order = (2, 4, 3, 5, 1, 6, 7)

    def own(s):
        a, b = lax.rem(s, 2), lax.rem(s, 3)
        rcv[b, me] = snd[a, me]
        rcv_st[b, me] = snd_st[a, me]

    def begin_in(s):
        for r in order:
            in_tokens(s, r, me).start()
        own(s)
        for r in order:
            in_stats(s, r, me).start()

    def end_in(s):
        for r in range(1, n):
            in_tokens(s, r, me).wait_send()
            in_stats(s, r, me).wait_send()
            in_tokens(s, r, peer(r)).wait_recv()
            in_stats(s, r, peer(r)).wait_recv()

    def begin_out(c):
        for r in order:
            out_copy(c, r, me).start()
        a, b = lax.rem(c, 2), lax.rem(c, 3)
        orcv[b, me] = osnd[a, me]

    def end_out(c):
        for r in range(1, n):
            out_copy(c, r, me).wait_send()
            out_copy(c, r, peer(r)).wait_recv()

    first = loads(0)
    for x in first:
        x.start()
    barrier = pltpu.get_barrier_semaphore()
    for r in range(1, n):
        pl.semaphore_signal(barrier, inc=1, device_id=(row, peer(r)), device_id_type=MESH)
    for a in range(5):
        first[a].wait()
        if a < 4:
            split(0, a)
        else:
            first[5].wait()
            stats(0)
        if a == 0:
            pl.semaphore_wait(barrier, n - 1)
        for b in {0: (0,), 1: ()}.get(a, (a - 1,)):
            for r in order:
                in_tokens(0, r, me, pl.ds(b * toks, toks)).start()
    own(0)
    for r in order:
        in_stats(0, r, me).start()
    for x in loads(1):
        x.start()

    def step(s, _):
        computes = s >= 1

        @pl.when(computes)
        def _():
            end_in(s - 1)

        @pl.when((s >= 3) & (s < chunks))
        def _():
            begin_in(s)

        @pl.when(s == chunks)
        def _():
            for r in order:
                near_copy(r, me).start()
            pltpu.make_async_copy(osnd.at[(chunks - 2) % 2, me], near_ref.at[me], nearsem).start()

        @pl.when(s >= 4)
        def _():
            for x in stores(s - 4):
                x.start()

        @pl.when(computes)
        def _():
            begin(s - 1)
            compute(s - 1, 0, n // 2)

        @pl.when(s >= 3)
        def _():
            end_out(s - 3)

        @pl.when((s >= 2) & (s < chunks))
        def _():
            begin_out(s - 2)

        @pl.when(computes)
        def _():
            compute(s - 1, n // 2, n)
            finish(s - 1)

        @pl.when(s + 1 < chunks)
        def _():
            for x in loads(s + 1):
                x.wait()
            prepare(s + 1)

        @pl.when(s < 2)
        def _():
            begin_in(s + 1)

        @pl.when(s + 2 < chunks)
        def _():
            for x in loads(s + 2):
                x.start()

        @pl.when(s >= 4)
        def _():
            for x in stores(s - 4):
                x.wait()

        @pl.when(s >= 3)
        def _():
            finalize(s - 3)
        return 0

    lax.fori_loop(0, chunks + 1, step, 0)

    tail = [pltpu.make_async_copy(osnd.at[(chunks - 1) % 2, peer(r)], x, lastsem.at[r])
            for r, x in zip(ORDER, last_refs)] + stores(chunks - 3)
    for x in tail:
        x.start()
    pltpu.make_async_copy(osnd.at[(chunks - 2) % 2, me], near_ref.at[me], nearsem).wait()
    for x in tail:
        x.wait()
    for r in range(1, n):
        near_copy(r, me).wait_send()
        near_copy(r, peer(r)).wait_recv()


def _merge(n, toks, at, dsts, part, stage, tmp, wsem):
    d = stage.shape[-1]
    piece = tmp.shape[0] // n
    writes = []
    for a in range(3):
        def block(i, _):
            rows = pl.ds(pl.multiple_of(a * toks + i * piece, piece), piece)
            for r in range(n):
                h, x = part(r, rows)
                tmp[pl.ds(h, piece, stride=n), :] = x.astype(F32)
            stage[a, pl.ds(pl.multiple_of(i * piece, piece), piece)] = (
                tmp[...].reshape(piece, n, d).astype(BF16))
            return 0
        lax.fori_loop(0, toks // piece, block, 0)
        writes.append(pltpu.make_async_copy(stage.at[a], dsts[a].at[:, at:at + n, :], wsem.at[a]))
        writes[-1].start()
    return writes


def _move_kernel(n, toks, rows, *refs):
    srcs, near, dsts, (buf, rsem, wsem, nbuf, stage, tmp, nsem, msem) = refs[:3], refs[3], refs[4:7], refs[7:]
    other = pltpu.make_async_copy(near, nbuf, nsem)
    other.start()
    slots = buf.shape[0]
    heads = srcs[0].shape[1]
    blocks = [(a, i) for i in range(srcs[0].shape[0] // rows) for a in range(3)]

    def read(t):
        a, i = blocks[t]
        return pltpu.make_async_copy(srcs[a].at[i * rows:(i + 1) * rows], buf.at[t % slots], rsem.at[t % slots])

    def write(t):
        a, i = blocks[t]
        return pltpu.make_async_copy(buf.at[t % slots], dsts[a].at[i * rows:(i + 1) * rows, 0:heads, :],
                                     wsem.at[t % slots])

    ahead = slots // 2
    for t in range(len(blocks) + ahead):
        if t < len(blocks):
            if t >= slots:
                write(t - slots).wait()
            read(t).start()
        if t >= ahead:
            read(t - ahead).wait()
            write(t - ahead).start()
        if t == len(blocks) // 2:
            other.wait()
            merged = _merge(n, toks, heads, dsts, lambda h, rows: (h, nbuf[h, rows, :]), stage, tmp, msem)
    for t in range(max(0, len(blocks) - slots), len(blocks)):
        write(t).wait()
    for x in merged:
        x.wait()


def _last_kernel(n, toks, *refs):
    parts, rest = refs[:n], refs[n + 3:]
    dsts, (stage, tmp, wsem) = rest[:3], rest[3:]
    heads = dsts[0].shape[1]
    me = lax.axis_index('cp')

    def part(i, rows):
        h = me
        for bit in (1, 2, 4):
            if ORDER[i] & bit:
                h = h + bit - 2 * bit * lax.rem(me // bit, 2)
        return h, parts[i][rows, :]

    for x in _merge(n, toks, heads - n, dsts, part, stage, tmp, wsem):
        x.wait()


def solution(mesh):
    n = mesh.shape['cp']
    spec = P('data', 'cp', None, None)
    lspec = P('data', None, 'cp')

    def local(q, k, v, o, lse, do):
        _, toks, heads, d = q.shape
        out = jax.ShapeDtypeStruct((toks, heads, d), BF16)
        early = jax.ShapeDtypeStruct((toks, heads - 2 * n, d), BF16)
        near = jax.ShapeDtypeStruct((n, 3 * toks, d), BF16)
        part = jax.ShapeDtypeStruct((3 * toks, d), BF16)
        any_ = pl.BlockSpec(memory_space=pl.ANY)
        dma = pltpu.SemaphoreType.DMA
        res = pl.pallas_call(
            functools.partial(_kernel, n, toks, heads),
            out_shape=(early,) * 3 + (near,) + (part,) * n,
            in_specs=[any_] * 6,
            out_specs=(any_,) * (4 + n),
            scratch_shapes=[
                pltpu.VMEM((5, toks, n, d), BF16),
                pltpu.VMEM((n, toks), F32),
                pltpu.VMEM((2, n, 4 * toks, d), BF16),
                pltpu.VMEM((2, n, 2, toks), F32),
                pltpu.VMEM((3, n, 4 * toks, d), BF16),
                pltpu.VMEM((3, n, 2, toks), F32),
                pltpu.VMEM((2, n, 3 * toks, d), BF16),
                pltpu.VMEM((3, n, 3 * toks, d), BF16),
                pltpu.VMEM((3, toks, n, d), BF16),
                pltpu.VMEM((toks // 4 * n, d), F32),
                pltpu.VMEM((n, d, toks), BF16),
                pltpu.VMEM((n, d, toks), F32),
                pltpu.VMEM((n, toks, d), F32),
                pltpu.VMEM((n, toks, d), F32),
                dma((2, n)), dma((3, n)), dma((2, n)), dma((3, n)), dma((2, n)), dma((3, n)),
                dma((5,)), dma, dma((3,)), dma((n,)), dma,
            ],
            compiler_params=pltpu.CompilerParams(
                collective_id=0, has_side_effects=True, vmem_limit_bytes=67_043_328),
        )(q[0], k[0], v[0], o[0], do[0], lse[0])
        moved = 2 * 3 * toks * (heads - n) * d * 2
        rows, slots = 32, 16
        dq, dk, dv = pl.pallas_call(
            functools.partial(_move_kernel, n, toks, rows),
            out_shape=(out, out, out),
            in_specs=[any_] * 4,
            out_specs=(any_,) * 3,
            scratch_shapes=[
                pltpu.VMEM((slots, rows, heads - 2 * n, d), BF16), dma((slots,)), dma((slots,)),
                pltpu.VMEM((n, 3 * toks, d), BF16), pltpu.VMEM((3, toks, n, d), BF16),
                pltpu.VMEM((toks // 4 * n, d), F32), dma, dma((3,)),
            ],
            cost_estimate=pl.CostEstimate(flops=0, bytes_accessed=moved, transcendentals=0),
        )(*res[:4])
        parts = [res[4]] + [lax.ppermute(x, 'cp', [(j, j ^ r) for j in range(n)])
                            for r, x in zip(ORDER[1:], res[5:])]
        dq, dk, dv = pl.pallas_call(
            functools.partial(_last_kernel, n, toks),
            out_shape=(out, out, out),
            in_specs=[pl.BlockSpec(memory_space=pltpu.VMEM)] * n + [any_] * 3,
            out_specs=(any_,) * 3,
            scratch_shapes=[
                pltpu.VMEM((3, toks, n, d), BF16), pltpu.VMEM((toks // 4 * n, d), F32), dma((3,)),
            ],
            input_output_aliases={n: 0, n + 1: 1, n + 2: 2},
            compiler_params=pltpu.CompilerParams(vmem_limit_bytes=12 << 20),
            cost_estimate=pl.CostEstimate(flops=0, bytes_accessed=12 * toks * n * d, transcendentals=0),
        )(*parts, dq, dk, dv)
        return dq[None], dk[None], dv[None]

    return jax.shard_map(local, mesh=mesh, in_specs=(spec, spec, spec, spec, lspec, spec),
                         out_specs=(spec, spec, spec), check_vma=False)
```

```python
import functools

import jax
import jax.numpy as jnp
from jax import lax
from jax.experimental import pallas as pl
from jax.experimental.pallas import tpu as pltpu
from jax.sharding import PartitionSpec as P

F32 = jnp.float32
BF16 = jnp.bfloat16
MESH = pl.DeviceIdType.MESH


ORDER = ((0, 0), (2, 4), (4, 2), (3, 5), (5, 3), (6, 6), (7, 7), (1, 1))


def _exchange(me, r):
    for bit in (1, 2, 4):
        if r & bit:
            me = me + bit - 2 * bit * lax.rem(me // bit, 2)
    return me


def _by_core(me, even, odd):
    return even + lax.rem(me, 2) * (odd - even)


NT = (((1,), (1,)), ((), ()))
NN = (((1,), (0,)), ((), ()))


def _dot(a, b, dims):
    return lax.dot_general(a, b, dims, preferred_element_type=F32)


def _kernel(n, toks, heads, q_ref, k_ref, v_ref, o_ref, do_ref, lse_ref, dq_ref, dk_ref, dv_ref, *rest):
    near_ref, last_refs, rest = rest[0], rest[1:n + 1], rest[n + 1:]
    (raw, raw_lse, snd, snd_st, rcv, rcv_st, osnd, orcv, ostage, tmp, kt, dqt, dka, dva,
            isend, irecv, ssend, srecv, osend, orecv, ldsem, lsesem, stsem, lastsem, nearsem) = rest
    half = toks // 2
    d = q_ref.shape[-1]
    scale = d ** -0.5
    chunks = heads // n
    me = lax.axis_index('cp')
    row = lax.axis_index('data')

    def peer(r):
        return _exchange(me, r)

    srcs = (q_ref, k_ref, v_ref, do_ref, o_ref)
    dsts = (dq_ref, dk_ref, dv_ref)

    def loads(c):
        h = pl.ds(pl.multiple_of(c * n, n), n)
        out = [pltpu.make_async_copy(x.at[:, h, :], raw.at[a], ldsem.at[a]) for a, x in enumerate(srcs)]
        out.append(pltpu.make_async_copy(lse_ref.at[h, :], raw_lse, lsesem))
        return out

    def stores(c):
        h = pl.ds(pl.multiple_of(c * n, n), n)
        return [pltpu.make_async_copy(ostage.at[a], x.at[:, h, :], stsem.at[a]) for a, x in enumerate(dsts)]

    def remote(src, dst, ssem, rsem, p):
        return pltpu.make_async_remote_copy(src_ref=src, dst_ref=dst, send_sem=ssem, recv_sem=rsem,
                                            device_id=(row, p), device_id_type=MESH)

    def in_tokens(s, r, at, rows=slice(None)):
        p = peer(r)
        a, b, par = lax.rem(s, 2), lax.rem(s, 3), lax.rem(s, 2)
        return remote(snd.at[a, p, rows], rcv.at[b, at, rows], isend.at[par, r], irecv.at[b, r], p)

    def in_stats(s, r, at):
        p = peer(r)
        a, b, par = lax.rem(s, 2), lax.rem(s, 3), lax.rem(s, 2)
        return remote(snd_st.at[a, p], rcv_st.at[b, at], ssend.at[par, r], srecv.at[b, r], p)

    def out_copy(c, r, at):
        p = peer(r)
        a, b, par = lax.rem(c, 2), lax.rem(c, 3), lax.rem(c, 2)
        return remote(osnd.at[a, p], orcv.at[b, at], osend.at[par, r], orecv.at[b, r], p)

    def near_copy(r, at):
        c = chunks - 2
        p = peer(r)
        return remote(osnd.at[c % 2, p], near_ref.at[at], osend.at[c % 2, r], orecv.at[c % 3, r], p)

    part = toks // 4

    def split(c, a):
        a_slot = lax.rem(c, 2)

        def piece(i, _):
            rows = pl.ds(pl.multiple_of(i * part, part), part)
            x = raw[a, rows].astype(F32).reshape(part * n, d)
            tmp[pl.ds(0, part * n), :] = x
            for h in range(n):
                snd[a_slot, h, pl.ds(pl.multiple_of(a * toks + i * part, part), part), :] = (
                    tmp[pl.ds(h, part, stride=n), :].astype(BF16))
            return 0
        lax.fori_loop(0, 4, piece, 0)

    def stats(c):
        a_slot = lax.rem(c, 2)
        for h in range(n):
            snd_st[a_slot, h, 0:1, :] = raw_lse[h:h + 1, :]

        def stat(i, _):
            rows = pl.ds(pl.multiple_of(i * part, part), part)
            x = raw[3, rows].astype(F32) * raw[4, rows].astype(F32)
            tmp[pl.ds(0, part * n), :] = x.reshape(part * n, d)
            for h in range(n):
                y = tmp[pl.ds(h, part, stride=n), :]
                snd_st[a_slot, h, 1:2, pl.ds(pl.multiple_of(i * part, part), part)] = (
                    jnp.sum(y.T, axis=0, keepdims=True))
            return 0
        lax.fori_loop(0, 4, stat, 0)

    def prepare(c):
        def tensor(a, _):
            split(c, a)
            return 0
        lax.fori_loop(0, 4, tensor, 0)
        stats(c)

    def finalize(c):
        b_slot = lax.rem(c, 3)

        def tensor(a, _):
            def piece(i, _):
                rows = pl.ds(pl.multiple_of(i * part, part), part)
                for h in range(n):
                    tmp[pl.ds(h, part, stride=n), :] = (
                        orcv[b_slot, h, pl.ds(pl.multiple_of(a * toks + i * part, part), part), :].astype(F32))
                ostage[a, rows] = tmp[pl.ds(0, part * n), :].reshape(part, n, d).astype(BF16)
                return 0
            return lax.fori_loop(0, 4, piece, 0)
        lax.fori_loop(0, 3, tensor, 0)

    def tile(b, i, q0, qn, j, k0, kn, mask):
        q = rcv[b, i, q0:q0 + qn, :]
        k = rcv[b, j, toks + k0:toks + k0 + kn, :]
        v = rcv[b, j, 2 * toks + k0:2 * toks + k0 + kn, :]
        do = rcv[b, i, 3 * toks + q0:3 * toks + q0 + qn, :]
        lse = rcv_st[b, i, 0:1, q0:q0 + qn]
        delta = rcv_st[b, i, 1:2, q0:q0 + qn]
        p = jnp.exp(_dot(k, q, NT) * scale - lse)
        if mask is not None:
            p = jnp.where(mask, p, 0.0)
        dp = _dot(v, do, NT)
        ds = (p * (dp - delta)).astype(BF16)
        dva[j, k0:k0 + kn, :] += _dot(p.astype(BF16), do, NN)
        dka[j, k0:k0 + kn, :] += _dot(ds, q, NN)
        dqt[i, :, q0:q0 + qn] += _dot(kt[j, :, k0:k0 + kn], ds, NN)

    def begin(c):
        b = lax.rem(c, 3)

        def clear(j, _):
            kt[j] = rcv[b, j, toks:2 * toks, :].T
            dqt[j] = jnp.zeros((d, toks), F32)
            dka[j] = jnp.zeros((toks, d), F32)
            dva[j] = jnp.zeros((toks, d), F32)
            return 0
        lax.fori_loop(0, n, clear, 0)

    def compute(c, lo, hi):
        b = lax.rem(c, 3)
        tri = (lax.broadcasted_iota(jnp.int32, (half, half), 0)
               <= lax.broadcasted_iota(jnp.int32, (half, half), 1))

        def keys(j, _):
            tile(b, j, 0, half, j, 0, half, tri)
            tile(b, j, half, half, j, 0, half, None)
            tile(b, j, half, half, j, half, half, tri)

            def lower(i, _):
                tile(b, i, half, half, j, 0, toks, None)
                return 0
            lax.fori_loop(0, j, lower, 0)

            def higher(i, _):
                tile(b, i, 0, toks, j, 0, half, None)
                return 0
            lax.fori_loop(j + 1, n, higher, 0)
            return 0
        lax.fori_loop(lo, hi, keys, 0)

    def finish(c):
        oslot = lax.rem(c, 2)

        def block(i, _):
            osnd[oslot, i, 0:toks, :] = (dqt[i].T * scale).astype(BF16)
            osnd[oslot, i, toks:2 * toks, :] = (dka[i] * scale).astype(BF16)
            osnd[oslot, i, 2 * toks:3 * toks, :] = dva[i].astype(BF16)
            return 0
        lax.fori_loop(0, n, block, 0)

    order = (2, 4, 3, 5, 1, 6, 7)

    def own(s):
        a, b = lax.rem(s, 2), lax.rem(s, 3)
        rcv[b, me] = snd[a, me]
        rcv_st[b, me] = snd_st[a, me]

    def begin_in(s):
        for r in order:
            in_tokens(s, r, me).start()
        own(s)
        for r in order:
            in_stats(s, r, me).start()

    def end_in(s):
        for r in range(1, n):
            in_tokens(s, r, me).wait_send()
            in_stats(s, r, me).wait_send()
            in_tokens(s, r, peer(r)).wait_recv()
            in_stats(s, r, peer(r)).wait_recv()

    def begin_out(c):
        for r in order:
            out_copy(c, r, me).start()
        a, b = lax.rem(c, 2), lax.rem(c, 3)
        orcv[b, me] = osnd[a, me]

    def end_out(c):
        for r in range(1, n):
            out_copy(c, r, me).wait_send()
            out_copy(c, r, peer(r)).wait_recv()

    first = loads(0)
    for x in first[:2]:
        x.start()
    barrier = pltpu.get_barrier_semaphore()
    for r in range(1, n):
        pl.semaphore_signal(barrier, inc=1, device_id=(row, peer(r)), device_id_type=MESH)
    for a in range(5):
        first[a].wait()
        if a == 0:
            for x in first[2:]:
                x.start()
        if a < 4:
            split(0, a)
        else:
            first[5].wait()
            stats(0)
        if a == 0:
            pl.semaphore_wait(barrier, n - 1)
        for b in {0: (0,), 1: ()}.get(a, (a - 1,)):
            for r in order:
                in_tokens(0, r, me, pl.ds(b * toks, toks)).start()
    own(0)
    for r in order:
        in_stats(0, r, me).start()
    for x in loads(1):
        x.start()

    def step(s, _):
        computes = s >= 1

        @pl.when(computes)
        def _():
            end_in(s - 1)

        @pl.when((s >= 3) & (s < chunks))
        def _():
            begin_in(s)

        @pl.when(s == chunks)
        def _():
            for r in order:
                near_copy(r, me).start()
            pltpu.make_async_copy(osnd.at[(chunks - 2) % 2, me], near_ref.at[me], nearsem).start()

        @pl.when(s >= 4)
        def _():
            for x in stores(s - 4):
                x.start()

        @pl.when(computes)
        def _():
            begin(s - 1)
            compute(s - 1, 0, n // 2)

        @pl.when(s >= 3)
        def _():
            end_out(s - 3)

        @pl.when((s >= 2) & (s < chunks))
        def _():
            begin_out(s - 2)

        @pl.when(computes)
        def _():
            compute(s - 1, n // 2, n)
            finish(s - 1)

        @pl.when(s + 1 < chunks)
        def _():
            for x in loads(s + 1):
                x.wait()
            prepare(s + 1)

        @pl.when(s < 2)
        def _():
            begin_in(s + 1)

        @pl.when(s + 2 < chunks)
        def _():
            for x in loads(s + 2):
                x.start()

        @pl.when(s >= 4)
        def _():
            for x in stores(s - 4):
                x.wait()

        @pl.when(s >= 3)
        def _():
            finalize(s - 3)
        return 0

    lax.fori_loop(0, chunks + 1, step, 0)

    tail = [pltpu.make_async_copy(osnd.at[(chunks - 1) % 2, _by_core(me, peer(r0), peer(r1))], x, lastsem.at[i])
            for i, ((r0, r1), x) in enumerate(zip(ORDER, last_refs))] + stores(chunks - 3)
    for x in tail:
        x.start()
    pltpu.make_async_copy(osnd.at[(chunks - 2) % 2, me], near_ref.at[me], nearsem).wait()
    for x in tail:
        x.wait()
    for r in range(1, n):
        near_copy(r, me).wait_send()
        near_copy(r, peer(r)).wait_recv()


def _merge(n, toks, at, dsts, part, stage, tmp, wsem):
    d = stage.shape[-1]
    piece = tmp.shape[0] // n
    writes = []
    for a in range(3):
        def block(i, _):
            rows = pl.ds(pl.multiple_of(a * toks + i * piece, piece), piece)
            for r in range(n):
                h, x = part(r, rows)
                tmp[pl.ds(h, piece, stride=n), :] = x.astype(F32)
            stage[a, pl.ds(pl.multiple_of(i * piece, piece), piece)] = (
                tmp[...].reshape(piece, n, d).astype(BF16))
            return 0
        lax.fori_loop(0, toks // piece, block, 0)
        writes.append(pltpu.make_async_copy(stage.at[a], dsts[a].at[:, at:at + n, :], wsem.at[a]))
        writes[-1].start()
    return writes


def _move_kernel(n, toks, rows, *refs):
    srcs, near, dsts, (buf, rsem, wsem, nbuf, stage, tmp, nsem, msem) = refs[:3], refs[3], refs[4:7], refs[7:]
    other = pltpu.make_async_copy(near, nbuf, nsem)
    other.start()
    slots = buf.shape[0]
    heads = srcs[0].shape[1]
    blocks = [(a, i) for i in range(srcs[0].shape[0] // rows) for a in range(3)]

    def read(t):
        a, i = blocks[t]
        return pltpu.make_async_copy(srcs[a].at[i * rows:(i + 1) * rows], buf.at[t % slots], rsem.at[t % slots])

    def write(t):
        a, i = blocks[t]
        return pltpu.make_async_copy(buf.at[t % slots], dsts[a].at[i * rows:(i + 1) * rows, 0:heads, :],
                                     wsem.at[t % slots])

    ahead = slots // 2
    for t in range(len(blocks) + ahead):
        if t < len(blocks):
            if t >= slots:
                write(t - slots).wait()
            read(t).start()
        if t >= ahead:
            read(t - ahead).wait()
            write(t - ahead).start()
        if t == len(blocks) // 2:
            other.wait()
            merged = _merge(n, toks, heads, dsts, lambda h, rows: (h, nbuf[h, rows, :]), stage, tmp, msem)
    for t in range(max(0, len(blocks) - slots), len(blocks)):
        write(t).wait()
    for x in merged:
        x.wait()


def _last_kernel(n, toks, *refs):
    parts, rest = refs[:n], refs[n + 3:]
    dsts, (stage, tmp, wsem) = rest[:3], rest[3:]
    heads = dsts[0].shape[1]
    me = lax.axis_index('cp')

    def part(i, rows):
        r0, r1 = ORDER[i]
        if r0 & 1:
            r0, r1 = r1, r0
        return _by_core(me, _exchange(me, r0), _exchange(me, r1)), parts[i][rows, :]

    for x in _merge(n, toks, heads - n, dsts, part, stage, tmp, wsem):
        x.wait()


def solution(mesh):
    n = mesh.shape['cp']
    spec = P('data', 'cp', None, None)
    lspec = P('data', None, 'cp')

    def local(q, k, v, o, lse, do):
        _, toks, heads, d = q.shape
        out = jax.ShapeDtypeStruct((toks, heads, d), BF16)
        early = jax.ShapeDtypeStruct((toks, heads - 2 * n, d), BF16)
        near = jax.ShapeDtypeStruct((n, 3 * toks, d), BF16)
        part = jax.ShapeDtypeStruct((3 * toks, d), BF16)
        any_ = pl.BlockSpec(memory_space=pl.ANY)
        dma = pltpu.SemaphoreType.DMA
        res = pl.pallas_call(
            functools.partial(_kernel, n, toks, heads),
            out_shape=(early,) * 3 + (near,) + (part,) * n,
            in_specs=[any_] * 6,
            out_specs=(any_,) * (4 + n),
            scratch_shapes=[
                pltpu.VMEM((5, toks, n, d), BF16),
                pltpu.VMEM((n, toks), F32),
                pltpu.VMEM((2, n, 4 * toks, d), BF16),
                pltpu.VMEM((2, n, 2, toks), F32),
                pltpu.VMEM((3, n, 4 * toks, d), BF16),
                pltpu.VMEM((3, n, 2, toks), F32),
                pltpu.VMEM((2, n, 3 * toks, d), BF16),
                pltpu.VMEM((3, n, 3 * toks, d), BF16),
                pltpu.VMEM((3, toks, n, d), BF16),
                pltpu.VMEM((toks // 4 * n, d), F32),
                pltpu.VMEM((n, d, toks), BF16),
                pltpu.VMEM((n, d, toks), F32),
                pltpu.VMEM((n, toks, d), F32),
                pltpu.VMEM((n, toks, d), F32),
                dma((2, n)), dma((3, n)), dma((2, n)), dma((3, n)), dma((2, n)), dma((3, n)),
                dma((5,)), dma, dma((3,)), dma((n,)), dma,
            ],
            compiler_params=pltpu.CompilerParams(
                collective_id=0, has_side_effects=True, vmem_limit_bytes=67_043_328),
        )(q[0], k[0], v[0], o[0], do[0], lse[0])
        moved = 2 * 3 * toks * (heads - n) * d * 2
        rows, slots = 32, 16
        dq, dk, dv = pl.pallas_call(
            functools.partial(_move_kernel, n, toks, rows),
            out_shape=(out, out, out),
            in_specs=[any_] * 4,
            out_specs=(any_,) * 3,
            scratch_shapes=[
                pltpu.VMEM((slots, rows, heads - 2 * n, d), BF16), dma((slots,)), dma((slots,)),
                pltpu.VMEM((n, 3 * toks, d), BF16), pltpu.VMEM((3, toks, n, d), BF16),
                pltpu.VMEM((toks // 4 * n, d), F32), dma, dma((3,)),
            ],
            cost_estimate=pl.CostEstimate(flops=0, bytes_accessed=moved, transcendentals=0),
        )(*res[:4])
        parts = [res[4]] + [lax.ppermute(x, 'cp', [(j, j ^ r[j % 2]) for j in range(n)])
                            for r, x in zip(ORDER[1:], res[5:])]
        dq, dk, dv = pl.pallas_call(
            functools.partial(_last_kernel, n, toks),
            out_shape=(out, out, out),
            in_specs=[pl.BlockSpec(memory_space=pltpu.VMEM)] * n + [any_] * 3,
            out_specs=(any_,) * 3,
            scratch_shapes=[
                pltpu.VMEM((3, toks, n, d), BF16), pltpu.VMEM((toks // 4 * n, d), F32), dma((3,)),
            ],
            input_output_aliases={n: 0, n + 1: 1, n + 2: 2},
            compiler_params=pltpu.CompilerParams(vmem_limit_bytes=12 << 20),
            cost_estimate=pl.CostEstimate(flops=0, bytes_accessed=12 * toks * n * d, transcendentals=0),
        )(*parts, dq, dk, dv)
        return dq[None], dk[None], dv[None]

    return jax.shard_map(local, mesh=mesh, in_specs=(spec, spec, spec, spec, lspec, spec),
                         out_specs=(spec, spec, spec), check_vma=False)
```

```python
import functools

import jax
import jax.numpy as jnp
from jax import lax
from jax.experimental import pallas as pl
from jax.experimental.pallas import tpu as pltpu
from jax.sharding import PartitionSpec as P

F32 = jnp.float32
BF16 = jnp.bfloat16
MESH = pl.DeviceIdType.MESH


ORDER = (0, 2, 4, 3, 5, 6, 7, 1)

NT = (((1,), (1,)), ((), ()))
NN = (((1,), (0,)), ((), ()))


def _dot(a, b, dims):
    return lax.dot_general(a, b, dims, preferred_element_type=F32)


def _kernel(n, toks, heads, q_ref, k_ref, v_ref, o_ref, do_ref, lse_ref, dq_ref, dk_ref, dv_ref, *rest):
    near_ref, last_refs, rest = rest[0], rest[1:n + 1], rest[n + 1:]
    (raw, raw_lse, snd, snd_st, rcv, rcv_st, osnd, orcv, ostage, tmp, kt, dqt, dka, dva,
            isend, irecv, ssend, srecv, osend, orecv, ldsem, lsesem, stsem, lastsem, nearsem) = rest
    half = toks // 2
    d = q_ref.shape[-1]
    scale = d ** -0.5
    chunks = heads // n
    me = lax.axis_index('cp')
    row = lax.axis_index('data')

    def peer(r):
        p = me
        if r & 1:
            p = p + 1 - 2 * lax.rem(me, 2)
        if r & 2:
            p = p + 2 - 4 * lax.rem(me // 2, 2)
        if r & 4:
            p = p + 4 - 8 * lax.rem(me // 4, 2)
        return p

    srcs = (q_ref, k_ref, v_ref, do_ref, o_ref)
    dsts = (dq_ref, dk_ref, dv_ref)

    def loads(c):
        h = pl.ds(pl.multiple_of(c * n, n), n)
        out = [pltpu.make_async_copy(x.at[:, h, :], raw.at[a], ldsem.at[a]) for a, x in enumerate(srcs)]
        out.append(pltpu.make_async_copy(lse_ref.at[h, :], raw_lse, lsesem))
        return out

    def stores(c):
        h = pl.ds(pl.multiple_of(c * n, n), n)
        return [pltpu.make_async_copy(ostage.at[a], x.at[:, h, :], stsem.at[a]) for a, x in enumerate(dsts)]

    def remote(src, dst, ssem, rsem, p):
        return pltpu.make_async_remote_copy(src_ref=src, dst_ref=dst, send_sem=ssem, recv_sem=rsem,
                                            device_id=(row, p), device_id_type=MESH)

    def in_tokens(s, r, at, rows=slice(None)):
        p = peer(r)
        a, b, par = lax.rem(s, 2), lax.rem(s, 3), lax.rem(s, 2)
        return remote(snd.at[a, p, rows], rcv.at[b, at, rows], isend.at[par, r], irecv.at[b, r], p)

    def in_stats(s, r, at):
        p = peer(r)
        a, b, par = lax.rem(s, 2), lax.rem(s, 3), lax.rem(s, 2)
        return remote(snd_st.at[a, p], rcv_st.at[b, at], ssend.at[par, r], srecv.at[b, r], p)

    def out_copy(c, r, at):
        p = peer(r)
        a, b, par = lax.rem(c, 2), lax.rem(c, 3), lax.rem(c, 2)
        return remote(osnd.at[a, p], orcv.at[b, at], osend.at[par, r], orecv.at[b, r], p)

    def near_copy(r, at):
        c = chunks - 2
        p = peer(r)
        return remote(osnd.at[c % 2, p], near_ref.at[at], osend.at[c % 2, r], orecv.at[c % 3, r], p)

    part = toks // 4

    def split(c, a):
        a_slot = lax.rem(c, 2)

        def piece(i, _):
            rows = pl.ds(pl.multiple_of(i * part, part), part)
            x = raw[a, rows].astype(F32).reshape(part * n, d)
            tmp[pl.ds(0, part * n), :] = x
            for h in range(n):
                snd[a_slot, h, pl.ds(pl.multiple_of(a * toks + i * part, part), part), :] = (
                    tmp[pl.ds(h, part, stride=n), :].astype(BF16))
            return 0
        lax.fori_loop(0, 4, piece, 0)

    def stats(c):
        a_slot = lax.rem(c, 2)
        for h in range(n):
            snd_st[a_slot, h, 0:1, :] = raw_lse[h:h + 1, :]

        def stat(i, _):
            rows = pl.ds(pl.multiple_of(i * part, part), part)
            x = raw[3, rows].astype(F32) * raw[4, rows].astype(F32)
            tmp[pl.ds(0, part * n), :] = x.reshape(part * n, d)
            for h in range(n):
                y = tmp[pl.ds(h, part, stride=n), :]
                snd_st[a_slot, h, 1:2, pl.ds(pl.multiple_of(i * part, part), part)] = (
                    jnp.sum(y.T, axis=0, keepdims=True))
            return 0
        lax.fori_loop(0, 4, stat, 0)

    def prepare(c):
        def tensor(a, _):
            split(c, a)
            return 0
        lax.fori_loop(0, 4, tensor, 0)
        stats(c)

    def finalize(c):
        b_slot = lax.rem(c, 3)

        def tensor(a, _):
            def piece(i, _):
                rows = pl.ds(pl.multiple_of(i * part, part), part)
                for h in range(n):
                    tmp[pl.ds(h, part, stride=n), :] = (
                        orcv[b_slot, h, pl.ds(pl.multiple_of(a * toks + i * part, part), part), :].astype(F32))
                ostage[a, rows] = tmp[pl.ds(0, part * n), :].reshape(part, n, d).astype(BF16)
                return 0
            return lax.fori_loop(0, 4, piece, 0)
        lax.fori_loop(0, 3, tensor, 0)

    def tile(b, i, q0, qn, j, k0, kn, mask):
        q = rcv[b, i, q0:q0 + qn, :]
        k = rcv[b, j, toks + k0:toks + k0 + kn, :]
        v = rcv[b, j, 2 * toks + k0:2 * toks + k0 + kn, :]
        do = rcv[b, i, 3 * toks + q0:3 * toks + q0 + qn, :]
        lse = rcv_st[b, i, 0:1, q0:q0 + qn]
        delta = rcv_st[b, i, 1:2, q0:q0 + qn]
        p = jnp.exp(_dot(k, q, NT) * scale - lse)
        if mask is not None:
            p = jnp.where(mask, p, 0.0)
        dp = _dot(v, do, NT)
        ds = (p * (dp - delta)).astype(BF16)
        dva[j, k0:k0 + kn, :] += _dot(p.astype(BF16), do, NN)
        dka[j, k0:k0 + kn, :] += _dot(ds, q, NN)
        dqt[i, :, q0:q0 + qn] += _dot(kt[j, :, k0:k0 + kn], ds, NN)

    def begin(c):
        b = lax.rem(c, 3)

        def clear(j, _):
            kt[j] = rcv[b, j, toks:2 * toks, :].T
            dqt[j] = jnp.zeros((d, toks), F32)
            dka[j] = jnp.zeros((toks, d), F32)
            dva[j] = jnp.zeros((toks, d), F32)
            return 0
        lax.fori_loop(0, n, clear, 0)

    def compute(c, lo, hi):
        b = lax.rem(c, 3)
        tri = (lax.broadcasted_iota(jnp.int32, (half, half), 0)
               <= lax.broadcasted_iota(jnp.int32, (half, half), 1))

        def keys(j, _):
            tile(b, j, 0, half, j, 0, half, tri)
            tile(b, j, half, half, j, 0, half, None)
            tile(b, j, half, half, j, half, half, tri)

            def lower(i, _):
                tile(b, i, half, half, j, 0, toks, None)
                return 0
            lax.fori_loop(0, j, lower, 0)

            def higher(i, _):
                tile(b, i, 0, toks, j, 0, half, None)
                return 0
            lax.fori_loop(j + 1, n, higher, 0)
            return 0
        lax.fori_loop(lo, hi, keys, 0)

    def finish(c):
        oslot = lax.rem(c, 2)

        def block(i, _):
            osnd[oslot, i, 0:toks, :] = (dqt[i].T * scale).astype(BF16)
            osnd[oslot, i, toks:2 * toks, :] = (dka[i] * scale).astype(BF16)
            osnd[oslot, i, 2 * toks:3 * toks, :] = dva[i].astype(BF16)
            return 0
        lax.fori_loop(0, n, block, 0)

    order = (2, 4, 3, 5, 1, 6, 7)

    def own(s):
        a, b = lax.rem(s, 2), lax.rem(s, 3)
        rcv[b, me] = snd[a, me]
        rcv_st[b, me] = snd_st[a, me]

    def begin_in(s):
        for r in order:
            in_tokens(s, r, me).start()
        own(s)
        for r in order:
            in_stats(s, r, me).start()

    def end_in(s):
        for r in range(1, n):
            in_tokens(s, r, me).wait_send()
            in_stats(s, r, me).wait_send()
            in_tokens(s, r, peer(r)).wait_recv()
            in_stats(s, r, peer(r)).wait_recv()

    def begin_out(c):
        for r in order:
            out_copy(c, r, me).start()
        a, b = lax.rem(c, 2), lax.rem(c, 3)
        orcv[b, me] = osnd[a, me]

    def end_out(c):
        for r in range(1, n):
            out_copy(c, r, me).wait_send()
            out_copy(c, r, peer(r)).wait_recv()

    first = loads(0)
    for x in first:
        x.start()
    barrier = pltpu.get_barrier_semaphore()
    for r in range(1, n):
        pl.semaphore_signal(barrier, inc=1, device_id=(row, peer(r)), device_id_type=MESH)
    for a in range(5):
        first[a].wait()
        if a < 4:
            split(0, a)
        else:
            first[5].wait()
            stats(0)
        if a == 0:
            pl.semaphore_wait(barrier, n - 1)
        for b in {0: (0,), 1: ()}.get(a, (a - 1,)):
            for r in order:
                in_tokens(0, r, me, pl.ds(b * toks, toks)).start()
    own(0)
    for r in order:
        in_stats(0, r, me).start()
    for x in loads(1):
        x.start()

    def step(s, _):
        computes = s >= 1

        @pl.when(computes)
        def _():
            end_in(s - 1)

        @pl.when((s >= 3) & (s < chunks))
        def _():
            begin_in(s)

        @pl.when(s == chunks)
        def _():
            for r in order:
                near_copy(r, me).start()
            pltpu.make_async_copy(osnd.at[(chunks - 2) % 2, me], near_ref.at[me], nearsem).start()

        @pl.when(s >= 4)
        def _():
            for x in stores(s - 4):
                x.start()

        @pl.when(computes)
        def _():
            begin(s - 1)
            compute(s - 1, 0, n // 2)

        @pl.when(s >= 3)
        def _():
            end_out(s - 3)

        @pl.when((s >= 2) & (s < chunks))
        def _():
            begin_out(s - 2)

        @pl.when(computes)
        def _():
            compute(s - 1, n // 2, n)
            finish(s - 1)

        @pl.when(s + 1 < chunks)
        def _():
            for x in loads(s + 1):
                x.wait()
            prepare(s + 1)

        @pl.when(s < 2)
        def _():
            begin_in(s + 1)

        @pl.when(s + 2 < chunks)
        def _():
            for x in loads(s + 2):
                x.start()

        @pl.when(s >= 4)
        def _():
            for x in stores(s - 4):
                x.wait()

        @pl.when(s >= 3)
        def _():
            finalize(s - 3)
        return 0

    lax.fori_loop(0, chunks + 1, step, 0)

    tail = [pltpu.make_async_copy(osnd.at[(chunks - 1) % 2, peer(r)], x, lastsem.at[r])
            for r, x in zip(ORDER, last_refs)] + stores(chunks - 3)
    for x in tail:
        x.start()
    pltpu.make_async_copy(osnd.at[(chunks - 2) % 2, me], near_ref.at[me], nearsem).wait()
    for x in tail:
        x.wait()
    for r in range(1, n):
        near_copy(r, me).wait_send()
        near_copy(r, peer(r)).wait_recv()


def _merge(n, toks, at, dsts, part, stage, tmp, wsem):
    d = stage.shape[-1]
    piece = tmp.shape[0] // n
    pieces = toks // piece

    def write(a, i):
        rows = pl.ds(pl.multiple_of(i * piece, piece), piece)
        return pltpu.make_async_copy(stage.at[a, rows], dsts[a].at[rows, at:at + n, :], wsem.at[a, i])

    for a in range(3):
        def block(i, _):
            rows = pl.ds(pl.multiple_of(a * toks + i * piece, piece), piece)
            for r in range(n):
                h, x = part(r, rows)
                tmp[pl.ds(h, piece, stride=n), :] = x.astype(F32)
            stage[a, pl.ds(pl.multiple_of(i * piece, piece), piece)] = (
                tmp[...].reshape(piece, n, d).astype(BF16))

            @pl.when(i > 0)
            def _():
                write(a, i - 1).start()
            return 0
        lax.fori_loop(0, pieces, block, 0)
        write(a, pieces - 1).start()
    return [write(a, i) for a in range(3) for i in range(pieces)]


def _move_kernel(n, toks, rows, *refs):
    srcs, near, dsts, (buf, rsem, wsem, nbuf, stage, tmp, nsem, msem) = refs[:3], refs[3], refs[4:7], refs[7:]
    other = pltpu.make_async_copy(near, nbuf, nsem)
    other.start()
    slots = buf.shape[0]
    heads = srcs[0].shape[1]
    blocks = [(a, i) for i in range(srcs[0].shape[0] // rows) for a in range(3)]

    def read(t):
        a, i = blocks[t]
        return pltpu.make_async_copy(srcs[a].at[i * rows:(i + 1) * rows], buf.at[t % slots], rsem.at[t % slots])

    def write(t):
        a, i = blocks[t]
        return pltpu.make_async_copy(buf.at[t % slots], dsts[a].at[i * rows:(i + 1) * rows, 0:heads, :],
                                     wsem.at[t % slots])

    ahead = slots // 2
    for t in range(len(blocks) + ahead):
        if t < len(blocks):
            if t >= slots:
                write(t - slots).wait()
            read(t).start()
        if t >= ahead:
            read(t - ahead).wait()
            write(t - ahead).start()
        if t == len(blocks) // 2:
            other.wait()
            merged = _merge(n, toks, heads, dsts, lambda h, rows: (h, nbuf[h, rows, :]), stage, tmp, msem)
    for t in range(max(0, len(blocks) - slots), len(blocks)):
        write(t).wait()
    for x in merged:
        x.wait()


def _last_kernel(n, toks, *refs):
    parts, rest = refs[:n], refs[n + 3:]
    dsts, (stage, tmp, wsem) = rest[:3], rest[3:]
    heads = dsts[0].shape[1]
    me = lax.axis_index('cp')

    def part(i, rows):
        h = me
        for bit in (1, 2, 4):
            if ORDER[i] & bit:
                h = h + bit - 2 * bit * lax.rem(me // bit, 2)
        return h, parts[i][rows, :]

    for x in _merge(n, toks, heads - n, dsts, part, stage, tmp, wsem):
        x.wait()


def solution(mesh):
    n = mesh.shape['cp']
    spec = P('data', 'cp', None, None)
    lspec = P('data', None, 'cp')

    def local(q, k, v, o, lse, do):
        _, toks, heads, d = q.shape
        out = jax.ShapeDtypeStruct((toks, heads, d), BF16)
        early = jax.ShapeDtypeStruct((toks, heads - 2 * n, d), BF16)
        near = jax.ShapeDtypeStruct((n, 3 * toks, d), BF16)
        part = jax.ShapeDtypeStruct((3 * toks, d), BF16)
        any_ = pl.BlockSpec(memory_space=pl.ANY)
        dma = pltpu.SemaphoreType.DMA
        res = pl.pallas_call(
            functools.partial(_kernel, n, toks, heads),
            out_shape=(early,) * 3 + (near,) + (part,) * n,
            in_specs=[any_] * 6,
            out_specs=(any_,) * (4 + n),
            scratch_shapes=[
                pltpu.VMEM((5, toks, n, d), BF16),
                pltpu.VMEM((n, toks), F32),
                pltpu.VMEM((2, n, 4 * toks, d), BF16),
                pltpu.VMEM((2, n, 2, toks), F32),
                pltpu.VMEM((3, n, 4 * toks, d), BF16),
                pltpu.VMEM((3, n, 2, toks), F32),
                pltpu.VMEM((2, n, 3 * toks, d), BF16),
                pltpu.VMEM((3, n, 3 * toks, d), BF16),
                pltpu.VMEM((3, toks, n, d), BF16),
                pltpu.VMEM((toks // 4 * n, d), F32),
                pltpu.VMEM((n, d, toks), BF16),
                pltpu.VMEM((n, d, toks), F32),
                pltpu.VMEM((n, toks, d), F32),
                pltpu.VMEM((n, toks, d), F32),
                dma((2, n)), dma((3, n)), dma((2, n)), dma((3, n)), dma((2, n)), dma((3, n)),
                dma((5,)), dma, dma((3,)), dma((n,)), dma,
            ],
            compiler_params=pltpu.CompilerParams(
                collective_id=0, has_side_effects=True, vmem_limit_bytes=67_043_328),
        )(q[0], k[0], v[0], o[0], do[0], lse[0])
        moved = 2 * 3 * toks * (heads - n) * d * 2
        rows, slots = 32, 16
        dq, dk, dv = pl.pallas_call(
            functools.partial(_move_kernel, n, toks, rows),
            out_shape=(out, out, out),
            in_specs=[any_] * 4,
            out_specs=(any_,) * 3,
            scratch_shapes=[
                pltpu.VMEM((slots, rows, heads - 2 * n, d), BF16), dma((slots,)), dma((slots,)),
                pltpu.VMEM((n, 3 * toks, d), BF16), pltpu.VMEM((3, toks, n, d), BF16),
                pltpu.VMEM((toks // 4 * n, d), F32), dma, dma((3, 4)),
            ],
            cost_estimate=pl.CostEstimate(flops=0, bytes_accessed=moved, transcendentals=0),
        )(*res[:4])
        parts = [res[4]] + [lax.ppermute(x, 'cp', [(j, j ^ r) for j in range(n)])
                            for r, x in zip(ORDER[1:], res[5:])]
        dq, dk, dv = pl.pallas_call(
            functools.partial(_last_kernel, n, toks),
            out_shape=(out, out, out),
            in_specs=[pl.BlockSpec(memory_space=pltpu.VMEM)] * n + [any_] * 3,
            out_specs=(any_,) * 3,
            scratch_shapes=[
                pltpu.VMEM((3, toks, n, d), BF16), pltpu.VMEM((toks // 4 * n, d), F32), dma((3, 4)),
            ],
            input_output_aliases={n: 0, n + 1: 1, n + 2: 2},
            compiler_params=pltpu.CompilerParams(vmem_limit_bytes=12 << 20),
            cost_estimate=pl.CostEstimate(flops=0, bytes_accessed=12 * toks * n * d, transcendentals=0),
        )(*parts, dq, dk, dv)
        return dq[None], dk[None], dv[None]

    return jax.shard_map(local, mesh=mesh, in_specs=(spec, spec, spec, spec, lspec, spec),
                         out_specs=(spec, spec, spec), check_vma=False)
```
